32 devices in a mesh: grp: 1, mid: 16 (over z, y, core), off: 2 (over x), sub: 1.
Axes of the slice: x: 2, y: 2, z: 4, core: 2. Of those that a mesh axis runs over, the one named last changes fastest.
Arguments:
- traces: bfloat16 [2, 1024, 1024], P('off', ('grp', 'mid'), 'sub'), may hold values from -6 to 6
- centre_offset: int32 [256], P(('grp', 'mid')), may hold values from 0 to 63
- foot_start: int32 [256, 16], P('grp'), may hold values from 0 to 240
- beam_count: int32 [16], P('grp'), may hold values from 2 to 16, as said below
- operator: bfloat16 [1024, 65536], P('sub', 'mid'), may hold values from -0.1875 to 0.1875
Outputs:
- image: float32 [256, 256], P(('grp', 'mid'))
The draws below stay inside these ranges and needn't reach their ends.
Inputs may be any that keep to these rules, and one draw needn't show every extreme that they name: `beam_count`: the live beams of all tiles sum to exactly 128, and the largest count is exactly 16.
All inputs are finite; a program needn't handle non-finite values.
Results may differ from the reference program's by a relative error of at most 0.0028.
Values may be sent and summed in bfloat16 or wider, within the bound.
No kernel may reach another device: no remote copies, remote signals or barrier semaphores. Data moves between devices by JAX's collectives and lax.ppermute only.
A program may use at most 64 MiB of HBM per device.

```python
import math
import jax
import jax.numpy as jnp
from jax import lax

NT = 1024
P_SIZE = 16
FL = 16
DEPTH = 256
HALF = 16
CB_DEV = 16
TR_DEV = 64
CENTRES = 256
TRACES = 1024
TILES = 16
LIVE = 128
OFFSETS = 2
FSUB = 512
FOOT = 4096
N_SUB = 1


def draw_foot_start(key, part):
    centre = jnp.arange(CENTRES, dtype=jnp.int32)[:, None]
    slope_index = jnp.arange(P_SIZE, dtype=jnp.int32)[None, :]
    drift = (2 * slope_index - P_SIZE + 1) * FL // (4 * P_SIZE)
    jitter = jax.random.randint(jax.random.fold_in(key, 7), (CENTRES, P_SIZE), -(FL // 2), FL // 2 + 1)
    return jnp.clip(centre - FL // 2 + drift + jitter, 0, CENTRES - FL).astype(jnp.int32)


def draw_centre_offset(key, part):
    slot = jnp.arange(CENTRES, dtype=jnp.int32) % CB_DEV
    reach = max(1, HALF // 2)
    anywhere = jax.random.randint(jax.random.fold_in(key, 11), (CENTRES,), 0, TR_DEV)
    lower = jax.random.randint(jax.random.fold_in(key, 12), (CENTRES,), 0, reach)
    upper = TR_DEV - 1 - jax.random.randint(jax.random.fold_in(key, 13), (CENTRES,), 0, reach)
    return jnp.where(slot == 0, lower, jnp.where(slot == 1, upper, anywhere)).astype(jnp.int32)


def draw_beam_count(key, part):
    order = jax.random.permutation(jax.random.fold_in(key, 21), TILES).astype(jnp.int32)
    rank = jnp.argsort(order, stable=True).astype(jnp.int32)
    spare = CB_DEV - 2
    remain = LIVE - CB_DEV - 2 * (TILES - 1)
    extra = jnp.clip(remain - (rank - 1) * spare, 0, spare)
    return jnp.where(rank == 0, CB_DEV, 2 + extra).astype(jnp.int32)


def shard_levels(key, extent, cuts, low, high):
    def one(dim, shards_of):
        draws = jax.random.uniform(jax.random.fold_in(jax.random.fold_in(key, 6), dim), (shards_of,), jnp.float32, low / len(cuts), high / len(cuts))
        return jnp.repeat(jnp.exp(draws), extent[dim] // shards_of).reshape((-1,) + (1,) * (len(extent) - dim - 1))

    factor_of = one(*cuts[0])
    for cut in cuts[1:]:
        factor_of = factor_of * one(*cut)
    return factor_of


def centred(rng, dims, deviation, bound, pieces=(), held_as=jnp.bfloat16):
    entries = deviation * jax.random.normal(rng, dims, jnp.float32)
    if pieces:
        entries = entries * shard_levels(rng, dims, pieces, -0.22, 0.18)
    return jnp.clip(entries, -bound, bound).astype(held_as)


def setup_inputs(seed: int = 0, part: int = 0) -> dict:
    streams_of = jax.random.split(jax.random.key(seed), 6)
    own_keys = jax.random.split(jax.random.fold_in(streams_of[5], part), 6)
    traces = centred(own_keys[0], (OFFSETS, TRACES, NT), 1.0, 6.0, ((0, 2), (1, 16)))
    centre_offset = draw_centre_offset(jax.random.fold_in(jax.random.fold_in(streams_of[5], part), 71), part)
    foot_start = draw_foot_start(jax.random.fold_in(jax.random.fold_in(streams_of[5], part), 71), part)
    beam_count = draw_beam_count(jax.random.fold_in(jax.random.fold_in(streams_of[5], part), 71), part)
    operator = centred(streams_of[4], (NT, P_SIZE * FOOT), NT ** -0.5, 0.1875, ((1, 16),))
    return {"traces": traces, "centre_offset": centre_offset, "foot_start": foot_start, "beam_count": beam_count, "operator": operator}


def dft_rows(first_row, row_count, freq_block):
    sample_index = first_row + jnp.arange(row_count, dtype=jnp.int32)[:, None]
    column = jnp.arange(NT, dtype=jnp.int32)[None, :]
    within = column % (2 * freq_block)
    frequency = column // (2 * freq_block) * freq_block + within % freq_block
    phase_angle = 2.0 * math.pi / NT * (sample_index * frequency % NT).astype(jnp.float32)
    values = jnp.where(within // freq_block == 1, -jnp.sin(phase_angle), jnp.cos(phase_angle))
    return values / math.sqrt(NT)

def slant_weights(frequency):
    offsets = jnp.arange(-HALF, HALF + 1, dtype=jnp.int32).astype(jnp.float32)
    taper = jnp.exp(-0.5 * (1.5 * offsets / HALF) ** 2)
    taper = taper / jnp.sqrt(jnp.sum(taper * taper))
    slopes = 0.25 * (jnp.arange(P_SIZE, dtype=jnp.int32).astype(jnp.float32) - 0.5 * (P_SIZE - 1))
    theta = 2.0 * math.pi / NT * slopes[:, None, None] * offsets[None, :, None] * frequency.astype(jnp.float32)[None, None, :]
    return (taper[None, :, None] * jnp.cos(theta), taper[None, :, None] * jnp.sin(theta))

def form_beams(windows_real, windows_imag, cos_weight, sin_weight):
    high = lax.Precision.HIGHEST
    beam_real = jnp.einsum('pxf,bxf->bpf', cos_weight, windows_real, precision=high) + jnp.einsum('pxf,bxf->bpf', sin_weight, windows_imag, precision=high)
    beam_imag = jnp.einsum('pxf,bxf->bpf', cos_weight, windows_imag, precision=high) - jnp.einsum('pxf,bxf->bpf', sin_weight, windows_real, precision=high)
    return (beam_real, beam_imag)

def live_rows(beam_count, per_tile, live_total):
    tile_ends = jnp.cumsum(beam_count).astype(jnp.int32)
    position = jnp.arange(live_total, dtype=jnp.int32)
    owner = lax.optimization_barrier(jnp.sum((position[:, None] >= tile_ends[None, :]).astype(jnp.int32), axis=1))
    first = tile_ends - beam_count.astype(jnp.int32)
    match = owner[:, None] == jnp.arange(beam_count.shape[0], dtype=jnp.int32)[None, :]
    chosen = lax.optimization_barrier(jnp.sum(jnp.where(match, first[None, :], 0), axis=1))
    return (owner * per_tile + position - chosen).astype(jnp.int32)

def reference(traces, centre_offset, foot_start, beam_count, operator):
    high = lax.Precision.HIGHEST
    dft_table = dft_rows(0, NT, FSUB)
    chosen = live_rows(beam_count, CB_DEV, LIVE)
    centre_trace = chosen // CB_DEV * TR_DEV + centre_offset[chosen]
    window_index = (centre_trace[:, None] + jnp.arange(2 * HALF + 1, dtype=jnp.int32)[None, :]).astype(jnp.int32)
    cos_weight, sin_weight = slant_weights(jnp.arange(NT // 2, dtype=jnp.int32))
    beam_sum = jnp.zeros((LIVE, P_SIZE, NT), jnp.float32)
    for offset_class in range(OFFSETS):
        spectra = jnp.dot(traces[offset_class].astype(jnp.float32), dft_table, precision=high)
        shaped = spectra.reshape(TRACES, N_SUB, 2, FSUB)
        real_all = jnp.pad(shaped[:, :, 0, :].reshape(TRACES, NT // 2), ((HALF, HALF), (0, 0)))
        imag_all = jnp.pad(shaped[:, :, 1, :].reshape(TRACES, NT // 2), ((HALF, HALF), (0, 0)))
        beam_real, beam_imag = form_beams(real_all[window_index], imag_all[window_index], cos_weight, sin_weight)
        stacked = jnp.stack([beam_real.reshape(LIVE, P_SIZE, N_SUB, FSUB), beam_imag.reshape(LIVE, P_SIZE, N_SUB, FSUB)], axis=3).reshape(LIVE, P_SIZE, NT)
        rounded = lax.optimization_barrier(stacked.astype(jnp.bfloat16))
        beam_sum = beam_sum + rounded.astype(jnp.float32)
    starts_live = foot_start[chosen]
    image = jnp.zeros((CENTRES, DEPTH), jnp.float32)
    lateral = jnp.arange(FL, dtype=jnp.int32)
    for slope in range(P_SIZE):
        kernel = operator[:, slope * FOOT:(slope + 1) * FOOT].astype(jnp.float32)
        footprint = jnp.dot(beam_sum[:, slope, :], kernel, precision=high)
        target = (starts_live[:, slope][:, None] + lateral[None, :]).reshape(-1)
        image = image.at[target].add(footprint.reshape(LIVE * FL, DEPTH))
    return image / math.sqrt(FL * P_SIZE)
```

```python
import functools
import math

import jax
import jax.numpy as jnp
import numpy as np
from jax import lax
from jax.experimental import pallas as pl
from jax.experimental.pallas import tpu as pltpu
from jax.sharding import PartitionSpec as P

NT = 1024
P_SIZE = 16
FL = 16
DEPTH = 256
HALF = 16
CB_DEV = 16
PAIRS = P_SIZE // 2
LANES = 128
GROUPS = 4
BF16 = jnp.bfloat16
F32 = jnp.float32


def split_bf16(values):
    high = values.astype(BF16)
    return high, (values - high.astype(values.dtype)).astype(BF16)


def quarter_table():
    phase = np.arange(NT // 4)[:, None] * np.arange(NT // 2)[None, :] % NT
    angle = 2.0 * np.pi / NT * phase
    table = np.concatenate([np.cos(angle), -np.sin(angle)], axis=1) / np.sqrt(NT)
    high = table.astype(BF16)
    return high, (table - high.astype(np.float64)).astype(BF16)


def offset_taper(offsets):
    window = np.exp(-0.5 * (1.5 * np.arange(-HALF, HALF + 1) / HALF) ** 2)
    return np.exp(-0.5 * (1.5 * offsets / HALF) ** 2) / np.sqrt(np.sum(window**2))


def slant_tables():
    offsets = np.arange(HALF + 1)
    slopes = 0.25 * (np.arange(PAIRS) - 0.5 * (P_SIZE - 1))
    theta = (
        2.0 * np.pi / NT * slopes[None, :, None] * offsets[:, None, None] * np.arange(NT // 2)[None, None, :]
    )
    weight = offset_taper(offsets)[:, None, None]
    cosine, sine = weight * np.cos(theta), weight * np.sin(theta)
    shape = (-1, PAIRS, NT // LANES, LANES)
    cosine = np.concatenate([cosine, cosine], axis=2).reshape(shape)
    sine = np.concatenate([sine, -sine], axis=2).reshape(shape)[1:]
    return cosine.astype(np.float32), sine.astype(np.float32)


def store_spectra(traces, high_ref, low_ref, spec_ref):
    quarter = high_ref.shape[0]
    parts = high_ref.shape[1] // LANES
    half = parts // 2
    rows = traces.shape[0]
    folded = jnp.concatenate([traces[:, q * quarter : (q + 1) * quarter] for q in range(4)], axis=0)
    turn = lax.broadcasted_iota(jnp.int32, (rows, LANES), 1) % 4
    odd = turn % 2 == 1
    flip_real = turn >= 2
    flip_imag = (turn == 1) | (turn == 2)
    product = jnp.dot(folded, high_ref[...], preferred_element_type=F32) + jnp.dot(
        folded, low_ref[...], preferred_element_type=F32
    )

    def turned(first, part):
        lanes = slice(part * LANES, (part + 1) * LANES)
        early = product[first * rows : (first + 1) * rows, lanes]
        late = product[(first + 2) * rows : (first + 3) * rows, lanes]
        return early + jnp.where(odd, -late, late)

    for part in range(half):
        real, imag = turned(1, part), turned(1, half + part)
        add_real, add_imag = jnp.where(odd, imag, real), jnp.where(odd, real, imag)
        spec_ref[pl.ds(part, rows, stride=parts), :] = turned(0, part) + jnp.where(
            flip_real, -add_real, add_real
        )
        spec_ref[pl.ds(half + part, rows, stride=parts), :] = turned(0, half + part) + jnp.where(
            flip_imag, -add_imag, add_imag
        )


def spectra_stage(own_hbm, high_hbm, low_hbm, spec_ref, high_ref, low_ref, own_ref, sems):
    pairs = [(own_hbm, own_ref), (high_hbm, high_ref), (low_hbm, low_ref)]
    copies = [pltpu.make_async_copy(src, dst, sems.at[i]) for i, (src, dst) in enumerate(pairs)]
    for copy in copies:
        copy.start()
    for copy in copies:
        copy.wait()
    store_spectra(own_ref[...], high_ref, low_ref, spec_ref)


def beams_stage(
    centre_hbm, count_hbm, cos_hbm, sin_hbm, own_spec_ref, within_ref, across_ref, high_ref, low_ref,
    out_ref, edge_ref, spec_ref, turned_ref, centre_ref, count_ref, cos_ref, sin_ref, sems,
):
    parts = cos_ref.shape[2]
    copies = [
        pltpu.make_async_copy(centre_hbm, centre_ref, sems.at[0]),
        pltpu.make_async_copy(count_hbm, count_ref, sems.at[1]),
        pltpu.make_async_copy(cos_hbm, cos_ref, sems.at[2]),
        pltpu.make_async_copy(sin_hbm, sin_ref, sems.at[3]),
    ]
    for copy in copies:
        copy.start()
    tile = lax.axis_index("mid")
    at_end = (tile == 0) | (tile == lax.axis_size("mid") - 1)
    within = within_ref[...].astype(F32)
    across = jnp.where(at_end, 0.0, across_ref[...].astype(F32))
    odd_tile = tile % 2 == 1
    above = jnp.where(odd_tile, within, across).astype(BF16)
    below = jnp.where(odd_tile, across, within).astype(BF16)
    edge = HALF * parts
    inner = own_spec_ref.shape[0]
    store_spectra(jnp.concatenate([above, below], axis=0), high_ref, low_ref, edge_ref)
    spec_ref[:edge] = edge_ref[:edge]
    spec_ref[edge : edge + inner] = own_spec_ref[...]
    spec_ref[edge + inner :] = edge_ref[edge:]
    for copy in copies:
        copy.wait()
    count = count_ref[tile]

    def row(index):
        return spec_ref[pl.ds(pl.multiple_of(index * parts, parts), parts), :]

    def one_beam(beam, carry):
        middle = centre_ref[beam] + HALF
        block = pl.ds(pl.multiple_of(beam * parts, parts), parts)

        @pl.when(beam < count)
        def _():
            centre = row(middle)
            even = [cos_ref[0, j] * centre for j in range(PAIRS)]
            odd_sum = [jnp.zeros_like(centre) for _ in range(PAIRS)]
            for x in range(1, HALF + 1):
                up, down = row(middle + x), row(middle - x)
                both = up + down
                swapped = pltpu.roll(up - down, parts // 2, 0)
                for j in range(PAIRS):
                    even[j] = even[j] + cos_ref[x, j] * both
                    odd_sum[j] = odd_sum[j] + sin_ref[x - 1, j] * swapped
            for j in range(PAIRS):
                turned_ref[j, block, :] = even[j] + odd_sum[j]
                turned_ref[P_SIZE - 1 - j, block, :] = even[j] - odd_sum[j]

        @pl.when(beam >= count)
        def _():
            for j in range(P_SIZE):
                turned_ref[j, block, :] = jnp.zeros((parts, LANES), F32)

        return carry

    lax.fori_loop(0, CB_DEV, one_beam, 0)
    for slope in range(P_SIZE):
        for part in range(parts):
            lanes = slice(part * LANES, (part + 1) * LANES)
            out_ref[slope, :, lanes] = turned_ref[slope, pl.ds(part, CB_DEV, stride=parts), :].astype(BF16)


def image_stage(place_ref, start_ref, beams_ref, operator_hbm, out_ref, operator_ref, sems, *, scale, copies):
    live = start_ref.shape[1]
    padded = place_ref.shape[1]
    groups, _, width = operator_ref.shape
    centres = out_ref.shape[0] * out_ref.shape[2]
    pieces = [
        pltpu.make_async_copy(
            operator_hbm.at[:, pl.ds(i * width, width)], operator_ref.at[i], sems.at[i]
        )
        for i in range(groups)
    ]
    for piece in pieces:
        piece.start()
    pick = (lax.broadcasted_iota(jnp.int32, (live, padded), 0) == place_ref[...]).astype(F32).astype(BF16)
    chosen = jnp.dot(pick, beams_ref[...], preferred_element_type=F32).astype(BF16)
    point = lax.broadcasted_iota(jnp.int32, (centres, live), 0) - start_ref[...]
    image = jnp.zeros((centres, DEPTH), F32)
    for group in range(groups):
        pieces[group].wait()
        for step in range(width // DEPTH):
            footprint = jnp.dot(
                chosen, operator_ref[group, :, step * DEPTH : (step + 1) * DEPTH], preferred_element_type=F32
            )
            high, low = split_bf16(footprint)
            hit = (point == group * (width // DEPTH) + step).astype(F32).astype(BF16)
            image = image + jnp.dot(
                jnp.concatenate([hit, hit], axis=1),
                jnp.concatenate([high, low], axis=0),
                preferred_element_type=F32,
            )
    image = (image * scale).astype(BF16)
    tile = out_ref.shape[2]
    for owner in range(out_ref.shape[0]):
        for copy in range(copies):
            out_ref[owner, copy] = image[owner * tile : (owner + 1) * tile]


VMEM = pl.BlockSpec(memory_space=pltpu.VMEM)
HBM = pl.BlockSpec(memory_space=pltpu.HBM)


def limit(mebibytes):
    return pltpu.CompilerParams(vmem_limit_bytes=mebibytes * 1024 * 1024)


def cost(flops, moved):
    return pl.CostEstimate(flops=flops, bytes_accessed=moved, transcendentals=0)


def in_hbm(array):
    return pltpu.with_memory_space_constraint(jnp.asarray(array), pltpu.HBM)


def shift(cells, axis, step):
    count = lax.axis_size(axis)
    return lax.ppermute(cells, axis, [(i, i + step) for i in range(count) if 0 <= i + step < count])


def beams_split_time(own, centre_offset, live_here):
    high = lax.Precision.HIGHEST
    sub_index = lax.axis_index("sub")
    samples = own.shape[1]
    freq_block = samples // 2
    sample_index = sub_index * samples + jnp.arange(samples, dtype=jnp.int32)[:, None]
    column = jnp.arange(NT, dtype=jnp.int32)[None, :]
    within = column % (2 * freq_block)
    frequency = column // (2 * freq_block) * freq_block + within % freq_block
    angle = 2.0 * math.pi / NT * (sample_index * frequency % NT).astype(F32)
    table = jnp.where(within // freq_block == 1, -jnp.sin(angle), jnp.cos(angle)) / math.sqrt(NT)
    partial_value = jnp.dot(own.astype(F32), table, precision=high)
    spectrum = lax.psum_scatter(partial_value, "sub", scatter_dimension=1, tiled=True)
    above = shift(spectrum[spectrum.shape[0] - HALF :], "mid", 1)
    below = shift(spectrum[:HALF], "mid", -1)
    padded = jnp.concatenate([above, spectrum, below], axis=0)
    windows = padded[centre_offset[:, None] + jnp.arange(2 * HALF + 1, dtype=jnp.int32)[None, :]]
    real, imag = windows[:, :, :freq_block], windows[:, :, freq_block:]
    offsets = np.arange(-HALF, HALF + 1)
    taper = jnp.asarray(offset_taper(offsets).astype(np.float32))[None, :, None]
    slopes = (0.25 * (np.arange(P_SIZE) - 0.5 * (P_SIZE - 1))).astype(np.float32)
    own_freq = (sub_index * freq_block + jnp.arange(freq_block, dtype=jnp.int32)).astype(F32)
    scale = (2.0 * math.pi / NT * slopes[:, None, None] * offsets[None, :, None]).astype(np.float32)
    theta = scale * own_freq[None, None, :]
    cosine, sine = taper * jnp.cos(theta), taper * jnp.sin(theta)
    add = functools.partial(jnp.einsum, "pxf,bxf->pbf", precision=high)
    beams = jnp.concatenate([add(cosine, real) + add(sine, imag), add(cosine, imag) - add(sine, real)], axis=2)
    alive = jnp.arange(CB_DEV, dtype=jnp.int32) < live_here
    return jnp.where(alive[None, :, None], beams, 0.0).astype(BF16)


def shards(traces, centre_offset, foot_start, beam_count, operator):
    mid_count = lax.axis_size("mid")
    off_count = lax.axis_size("off")
    sub_count = lax.axis_size("sub")
    mid_index = lax.axis_index("mid")
    samples = traces.shape[2]
    own = traces[0]
    counts = beam_count.astype(jnp.int32)
    tiles = jnp.arange(mid_count, dtype=jnp.int32)
    if sub_count == 1:
        odd_tile = mid_index % 2 == 1
        head, tail = own[:HALF], own[own.shape[0] - HALF :]
        ends = [(0, 0), (mid_count - 1, mid_count - 1)]
        inner_pairs = [(i, i - 1 if i % 2 == 0 else i + 1) for i in range(1, mid_count - 1)]
        within = lax.ppermute(jnp.where(odd_tile, head, tail), "mid", [(i, i ^ 1) for i in range(mid_count)])
        across = lax.ppermute(jnp.where(odd_tile, tail, head), "mid", ends + inner_pairs)
        table = quarter_table()
        slant = slant_tables()
        parts = samples // LANES
        inner = own.shape[0] * parts
        edge = 2 * HALF * parts
        spec, high, low = pl.pallas_call(
            spectra_stage,
            out_shape=[pltpu.VMEM((inner, LANES), F32)] + [pltpu.VMEM(t.shape, t.dtype) for t in table],
            in_specs=[HBM] * 3,
            out_specs=[VMEM] * 3,
            scratch_shapes=[pltpu.VMEM(own.shape, BF16), pltpu.SemaphoreType.DMA((3,))],
            compiler_params=limit(16),
            cost_estimate=cost(4 * 10**9, 4 * 10**6),
            name="spectra",
        )(in_hbm(own), *(in_hbm(t) for t in table))
        beams = pl.pallas_call(
            beams_stage,
            out_shape=pltpu.VMEM((P_SIZE, CB_DEV, samples), BF16),
            in_specs=[HBM] * 4 + [VMEM] * 5,
            out_specs=VMEM,
            scratch_shapes=[
                pltpu.VMEM((edge, LANES), F32),
                pltpu.VMEM((edge + inner, LANES), F32),
                pltpu.VMEM((P_SIZE, CB_DEV * parts, LANES), F32),
                pltpu.SMEM(centre_offset.shape, jnp.int32),
                pltpu.SMEM(beam_count.shape, jnp.int32),
            ]
            + [pltpu.VMEM(t.shape, t.dtype) for t in slant]
            + [pltpu.SemaphoreType.DMA((4,))],
            compiler_params=limit(16),
            cost_estimate=cost(4 * 10**9, 4 * 10**6),
            name="beams",
        )(in_hbm(centre_offset), in_hbm(counts), *(in_hbm(t) for t in slant), spec, within, across, high, low)
    else:
        live_here = jnp.sum(jnp.where(tiles == mid_index, counts, 0))
        beams = beams_split_time(own, centre_offset, live_here)
    shares = mid_count // P_SIZE
    if shares > 1:
        beams = jnp.repeat(beams, shares, axis=0)
    received = lax.all_to_all(
        beams.reshape(mid_count * CB_DEV, samples), "mid", split_axis=0, concat_axis=0, tiled=True
    )
    columns = operator.shape[1]
    footprint_size = FL * DEPTH
    first_column = mid_index * columns
    slope = first_column // footprint_size
    lateral_first = first_column % footprint_size // DEPTH
    rows = mid_count * CB_DEV
    live_total = rows // 2
    before = jnp.sum(jnp.where(tiles[None, :] < tiles[:, None], counts[None, :], 0), axis=1)
    slot = jnp.arange(CB_DEV, dtype=jnp.int32)
    place = jnp.where(slot[None, :] < counts[:, None], before[:, None] + slot[None, :], -1).reshape(1, rows)
    starts = lax.dynamic_index_in_dim(foot_start, slope, 1, keepdims=False)
    position = jnp.arange(live_total, dtype=jnp.int32)
    live_starts = jnp.sum(
        jnp.where(place.reshape(rows, 1) == position[None, :], starts[:, None], 0), axis=0
    )
    live_starts = (live_starts + lateral_first).reshape(1, live_total)
    partial_image = pl.pallas_call(
        functools.partial(image_stage, scale=1.0 / math.sqrt(FL * P_SIZE), copies=off_count),
        out_shape=jax.ShapeDtypeStruct((mid_count, off_count, CB_DEV, DEPTH), BF16),
        in_specs=[VMEM] * 3 + [HBM],
        out_specs=VMEM,
        scratch_shapes=[
            pltpu.VMEM((GROUPS, samples, columns // GROUPS), BF16),
            pltpu.SemaphoreType.DMA((GROUPS,)),
        ],
        compiler_params=limit(24),
        cost_estimate=cost(2 * 10**9, 10**7),
        name="image",
    )(place, live_starts, received, in_hbm(operator))
    parts = lax.all_to_all(
        partial_image.reshape(mid_count * off_count * CB_DEV, DEPTH),
        ("mid", "off"),
        split_axis=0,
        concat_axis=0,
        tiled=True,
    )
    image = jnp.sum(parts.reshape(mid_count * off_count, CB_DEV, DEPTH).astype(F32), axis=0)
    if sub_count > 1:
        image = lax.psum(image, "sub")
    return image


def solution(mesh):
    return jax.shard_map(
        shards,
        mesh=mesh,
        in_specs=(
            P("off", ("grp", "mid"), "sub"),
            P(("grp", "mid")),
            P("grp", None),
            P("grp"),
            P("sub", "mid"),
        ),
        out_specs=P(("grp", "mid"), None),
        check_vma=False,
    )
```

```python
import functools
import math

import jax
import jax.numpy as jnp
import numpy as np
from jax import lax
from jax.experimental import pallas as pl
from jax.experimental.pallas import tpu as pltpu
from jax.sharding import PartitionSpec as P

NT = 1024
P_SIZE = 16
FL = 16
DEPTH = 256
HALF = 16
CB_DEV = 16
PAIRS = P_SIZE // 2
LANES = 128
PIECES = 4
BF16 = jnp.bfloat16
F32 = jnp.float32


def split_bf16(values):
    high = values.astype(BF16)
    return high, (values - high.astype(values.dtype)).astype(BF16)


def quarter_table():
    phase = np.arange(NT // 4)[:, None] * np.arange(NT // 2)[None, :] % NT
    angle = 2.0 * np.pi / NT * phase
    table = np.concatenate([np.cos(angle), -np.sin(angle)], axis=1) / np.sqrt(NT)
    high = table.astype(BF16)
    return high, (table - high.astype(np.float64)).astype(BF16)


def offset_taper(offsets):
    window = np.exp(-0.5 * (1.5 * np.arange(-HALF, HALF + 1) / HALF) ** 2)
    return np.exp(-0.5 * (1.5 * offsets / HALF) ** 2) / np.sqrt(np.sum(window**2))


def slant_tables():
    offsets = np.arange(HALF + 1)
    slopes = 0.25 * (np.arange(PAIRS) - 0.5 * (P_SIZE - 1))
    theta = (
        2.0 * np.pi / NT * slopes[None, :, None] * offsets[:, None, None] * np.arange(NT // 2)[None, None, :]
    )
    weight = offset_taper(offsets)[:, None, None]
    cosine, sine = weight * np.cos(theta), weight * np.sin(theta)
    shape = (-1, PAIRS, NT // LANES, LANES)
    cosine = np.concatenate([cosine, cosine], axis=2).reshape(shape)
    sine = np.concatenate([sine, -sine], axis=2).reshape(shape)[1:]
    return cosine.astype(np.float32), sine.astype(np.float32)


def store_spectra(traces, high_ref, low_ref, spec_ref):
    quarter = high_ref.shape[0]
    parts = high_ref.shape[1] // LANES
    half = parts // 2
    rows = traces.shape[0]
    folded = jnp.concatenate([traces[:, q * quarter : (q + 1) * quarter] for q in range(4)], axis=0)
    turn = lax.broadcasted_iota(jnp.int32, (rows, LANES), 1) % 4
    odd = turn % 2 == 1
    flip_real = turn >= 2
    flip_imag = (turn == 1) | (turn == 2)
    product = jnp.dot(folded, high_ref[...], preferred_element_type=F32) + jnp.dot(
        folded, low_ref[...], preferred_element_type=F32
    )

    def turned(first, part):
        lanes = slice(part * LANES, (part + 1) * LANES)
        early = product[first * rows : (first + 1) * rows, lanes]
        late = product[(first + 2) * rows : (first + 3) * rows, lanes]
        return early + jnp.where(odd, -late, late)

    for part in range(half):
        real, imag = turned(1, part), turned(1, half + part)
        add_real, add_imag = jnp.where(odd, imag, real), jnp.where(odd, real, imag)
        spec_ref[pl.ds(part, rows, stride=parts), :] = turned(0, part) + jnp.where(
            flip_real, -add_real, add_real
        )
        spec_ref[pl.ds(half + part, rows, stride=parts), :] = turned(0, half + part) + jnp.where(
            flip_imag, -add_imag, add_imag
        )


def live_layout(counts, starts, live):
    padded = starts.shape[1]
    beam = lax.broadcasted_iota(jnp.int32, (1, padded), 1)
    place = jnp.full((1, padded), -1, jnp.int32)
    before = jnp.int32(0)
    for tile in range(padded // CB_DEV):
        slot = beam - tile * CB_DEV
        here = (slot >= 0) & (slot < counts[tile])
        place = jnp.where(here, before + slot, place)
        before = before + counts[tile]
    pick = (lax.broadcasted_iota(jnp.int32, (live, padded), 0) == place).astype(F32).astype(BF16)
    row = lax.broadcasted_iota(jnp.int32, (8, padded), 0)
    digits = jnp.where(row == 0, starts % CB_DEV, jnp.where(row == 1, starts // CB_DEV, 0))
    digits = lax.dot_general(
        digits.astype(F32).astype(BF16), pick, (((1,), (1,)), ((), ())), preferred_element_type=F32
    )
    return place, (digits[0:1] + CB_DEV * digits[1:2]).astype(jnp.int32)


def half_columns(operator_hbm, held_ref, half):
    depth, width = held_ref.shape[0] // PIECES, held_ref.shape[1]
    blocks = [pl.ds(piece * depth, depth) for piece in range(PIECES)]
    return [(operator_hbm.at[rows, pl.ds(half * width, width)], held_ref.at[rows]) for rows in blocks]


def first_stage(
    own_hbm, high_hbm, low_hbm, count_hbm, point_hbm, cos_hbm, sin_hbm, operator_hbm,
    spec_ref, high_ref, low_ref, cos_ref, sin_ref, operator_ref, place_ref, start_ref,
    own_ref, count_ref, point_ref, sems,
):
    pairs = [
        (own_hbm, own_ref), (high_hbm, high_ref), (low_hbm, low_ref), (count_hbm, count_ref),
        (point_hbm, point_ref), (cos_hbm, cos_ref), (sin_hbm, sin_ref),
    ]
    pairs += half_columns(operator_hbm, operator_ref, 0)
    copies = [pltpu.make_async_copy(src, dst, sems.at[i]) for i, (src, dst) in enumerate(pairs)]
    for copy in copies:
        copy.start()
    for copy in copies[:5]:
        copy.wait()
    store_spectra(own_ref[...], high_ref, low_ref, spec_ref)
    first_column = lax.axis_index("mid") * operator_hbm.shape[1]
    slope = first_column // (FL * DEPTH)
    rows = lax.broadcasted_iota(jnp.int32, point_ref.shape, 0)
    starts = jnp.sum(jnp.where(rows == slope, point_ref[...], 0), axis=0, keepdims=True)
    place, live_starts = live_layout(count_ref, starts, start_ref.shape[1])
    place_ref[...] = place
    start_ref[...] = live_starts + first_column % (FL * DEPTH) // DEPTH
    for copy in copies[5:]:
        copy.wait()


def beams_stage(
    centre_hbm, count_hbm, operator_hbm, own_spec_ref, within_ref, across_ref, high_ref, low_ref, cos_ref, sin_ref,
    out_ref, held_ref, edge_ref, spec_ref, turned_ref, centre_ref, count_ref, sems,
):
    parts = cos_ref.shape[2]
    pairs = [(centre_hbm, centre_ref), (count_hbm, count_ref)] + half_columns(operator_hbm, held_ref, 1)
    copies = [pltpu.make_async_copy(src, dst, sems.at[i]) for i, (src, dst) in enumerate(pairs)]
    for copy in copies:
        copy.start()
    tile = lax.axis_index("mid")
    at_end = (tile == 0) | (tile == lax.axis_size("mid") - 1)
    within = within_ref[...].astype(F32)
    across = jnp.where(at_end, 0.0, across_ref[...].astype(F32))
    odd_tile = tile % 2 == 1
    above = jnp.where(odd_tile, within, across).astype(BF16)
    below = jnp.where(odd_tile, across, within).astype(BF16)
    edge = HALF * parts
    inner = own_spec_ref.shape[0]
    store_spectra(jnp.concatenate([above, below], axis=0), high_ref, low_ref, edge_ref)
    spec_ref[:edge] = edge_ref[:edge]
    spec_ref[edge : edge + inner] = own_spec_ref[...]
    spec_ref[edge + inner :] = edge_ref[edge:]
    for copy in copies[:2]:
        copy.wait()
    count = count_ref[tile]

    def row(index):
        return spec_ref[pl.ds(pl.multiple_of(index * parts, parts), parts), :]

    def one_beam(beam, carry):
        middle = centre_ref[beam] + HALF
        block = pl.ds(pl.multiple_of(beam * parts, parts), parts)

        @pl.when(beam < count)
        def _():
            centre = row(middle)
            even = [cos_ref[0, j] * centre for j in range(PAIRS)]
            odd_sum = [jnp.zeros_like(centre) for _ in range(PAIRS)]
            for x in range(1, HALF + 1):
                up, down = row(middle + x), row(middle - x)
                both = up + down
                swapped = pltpu.roll(up - down, parts // 2, 0)
                for j in range(PAIRS):
                    even[j] = even[j] + cos_ref[x, j] * both
                    odd_sum[j] = odd_sum[j] + sin_ref[x - 1, j] * swapped
            for j in range(PAIRS):
                turned_ref[j, block, :] = even[j] + odd_sum[j]
                turned_ref[P_SIZE - 1 - j, block, :] = even[j] - odd_sum[j]

        @pl.when(beam >= count)
        def _():
            for j in range(P_SIZE):
                turned_ref[j, block, :] = jnp.zeros((parts, LANES), F32)

        return carry

    lax.fori_loop(0, CB_DEV, one_beam, 0)
    for slope in range(P_SIZE):
        for part in range(parts):
            lanes = slice(part * LANES, (part + 1) * LANES)
            out_ref[slope, :, lanes] = turned_ref[slope, pl.ds(part, CB_DEV, stride=parts), :].astype(BF16)
    for copy in copies[2:]:
        copy.wait()


def image_stage(place_ref, start_ref, beams_ref, early_ref, late_ref, out_ref, *, scale, copies):
    live = start_ref.shape[1]
    padded = place_ref.shape[1]
    half = early_ref.shape[1] // DEPTH
    centres = out_ref.shape[0] * out_ref.shape[2]
    pick = (lax.broadcasted_iota(jnp.int32, (live, padded), 0) == place_ref[...]).astype(F32).astype(BF16)
    chosen = jnp.dot(pick, beams_ref[...], preferred_element_type=F32).astype(BF16)
    point = lax.broadcasted_iota(jnp.int32, (centres, live), 0) - start_ref[...]
    image = jnp.zeros((centres, DEPTH), F32)
    for step in range(2 * half):
        columns = slice(step % half * DEPTH, (step % half + 1) * DEPTH)
        operator_ref = early_ref if step < half else late_ref
        footprint = jnp.dot(chosen, operator_ref[:, columns], preferred_element_type=F32)
        high, low = split_bf16(footprint)
        hit = (point == step).astype(F32).astype(BF16)
        image = image + jnp.dot(
            jnp.concatenate([hit, hit], axis=1),
            jnp.concatenate([high, low], axis=0),
            preferred_element_type=F32,
        )
    image = (image * scale).astype(BF16)
    tile = out_ref.shape[2]
    for owner in range(out_ref.shape[0]):
        for copy in range(copies):
            out_ref[owner, copy] = image[owner * tile : (owner + 1) * tile]


VMEM = pl.BlockSpec(memory_space=pltpu.VMEM)
HBM = pl.BlockSpec(memory_space=pltpu.HBM)


def limit(mebibytes):
    return pltpu.CompilerParams(vmem_limit_bytes=mebibytes * 1024 * 1024)


def cost(flops, moved):
    return pl.CostEstimate(flops=flops, bytes_accessed=moved, transcendentals=0)


def in_hbm(array):
    return pltpu.with_memory_space_constraint(jnp.asarray(array), pltpu.HBM)


def shift(cells, axis, step):
    count = lax.axis_size(axis)
    return lax.ppermute(cells, axis, [(i, i + step) for i in range(count) if 0 <= i + step < count])


def beams_split_time(own, centre_offset, live_here):
    high = lax.Precision.HIGHEST
    sub_index = lax.axis_index("sub")
    samples = own.shape[1]
    freq_block = samples // 2
    sample_index = sub_index * samples + jnp.arange(samples, dtype=jnp.int32)[:, None]
    column = jnp.arange(NT, dtype=jnp.int32)[None, :]
    within = column % (2 * freq_block)
    frequency = column // (2 * freq_block) * freq_block + within % freq_block
    angle = 2.0 * math.pi / NT * (sample_index * frequency % NT).astype(F32)
    table = jnp.where(within // freq_block == 1, -jnp.sin(angle), jnp.cos(angle)) / math.sqrt(NT)
    partial_value = jnp.dot(own.astype(F32), table, precision=high)
    spectrum = lax.psum_scatter(partial_value, "sub", scatter_dimension=1, tiled=True)
    above = shift(spectrum[spectrum.shape[0] - HALF :], "mid", 1)
    below = shift(spectrum[:HALF], "mid", -1)
    padded = jnp.concatenate([above, spectrum, below], axis=0)
    windows = padded[centre_offset[:, None] + jnp.arange(2 * HALF + 1, dtype=jnp.int32)[None, :]]
    real, imag = windows[:, :, :freq_block], windows[:, :, freq_block:]
    offsets = np.arange(-HALF, HALF + 1)
    taper = jnp.asarray(offset_taper(offsets).astype(np.float32))[None, :, None]
    slopes = (0.25 * (np.arange(P_SIZE) - 0.5 * (P_SIZE - 1))).astype(np.float32)
    own_freq = (sub_index * freq_block + jnp.arange(freq_block, dtype=jnp.int32)).astype(F32)
    scale = (2.0 * math.pi / NT * slopes[:, None, None] * offsets[None, :, None]).astype(np.float32)
    theta = scale * own_freq[None, None, :]
    cosine, sine = taper * jnp.cos(theta), taper * jnp.sin(theta)
    add = functools.partial(jnp.einsum, "pxf,bxf->pbf", precision=high)
    beams = jnp.concatenate([add(cosine, real) + add(sine, imag), add(cosine, imag) - add(sine, real)], axis=2)
    alive = jnp.arange(CB_DEV, dtype=jnp.int32) < live_here
    return jnp.where(alive[None, :, None], beams, 0.0).astype(BF16)


def shards(traces, centre_offset, foot_start, beam_count, operator):
    mid_count = lax.axis_size("mid")
    off_count = lax.axis_size("off")
    sub_count = lax.axis_size("sub")
    mid_index = lax.axis_index("mid")
    samples = traces.shape[2]
    own = traces[0]
    counts = beam_count.astype(jnp.int32)
    tiles = jnp.arange(mid_count, dtype=jnp.int32)
    rows = mid_count * CB_DEV
    live_total = rows // 2
    if sub_count == 1:
        odd_tile = mid_index % 2 == 1
        head, tail = own[:HALF], own[own.shape[0] - HALF :]
        ends = [(0, 0), (mid_count - 1, mid_count - 1)]
        inner_pairs = [(i, i - 1 if i % 2 == 0 else i + 1) for i in range(1, mid_count - 1)]
        within = lax.ppermute(jnp.where(odd_tile, head, tail), "mid", [(i, i ^ 1) for i in range(mid_count)])
        across = lax.ppermute(jnp.where(odd_tile, tail, head), "mid", ends + inner_pairs)
        tables = quarter_table() + slant_tables()
        parts = samples // LANES
        inner = own.shape[0] * parts
        edge = 2 * HALF * parts
        half_shape = (operator.shape[0], operator.shape[1] // 2)
        spec, high, low, cosine, sine, operator_early, place, live_starts = pl.pallas_call(
            first_stage,
            out_shape=[pltpu.VMEM((inner, LANES), F32)]
            + [pltpu.VMEM(t.shape, t.dtype) for t in tables]
            + [pltpu.VMEM(half_shape, BF16)]
            + [pltpu.VMEM((1, n), jnp.int32) for n in (rows, live_total)],
            in_specs=[HBM] * 8,
            out_specs=[VMEM] * 8,
            scratch_shapes=[
                pltpu.VMEM(own.shape, BF16),
                pltpu.SMEM(counts.shape, jnp.int32),
                pltpu.VMEM((P_SIZE, rows), jnp.int32),
                pltpu.SemaphoreType.DMA((7 + PIECES,)),
            ],
            compiler_params=limit(16),
            cost_estimate=cost(4 * 10**9, 10**7),
            name="first",
        )(*(in_hbm(t) for t in (own,) + tables[:2] + (counts, foot_start.T) + tables[2:] + (operator,)))
        beams, operator_late = pl.pallas_call(
            beams_stage,
            out_shape=[pltpu.VMEM((P_SIZE, CB_DEV, samples), BF16), pltpu.VMEM(half_shape, BF16)],
            in_specs=[HBM] * 3 + [VMEM] * 7,
            out_specs=[VMEM] * 2,
            scratch_shapes=[
                pltpu.VMEM((edge, LANES), F32),
                pltpu.VMEM((edge + inner, LANES), F32),
                pltpu.VMEM((P_SIZE, CB_DEV * parts, LANES), F32),
                pltpu.SMEM(centre_offset.shape, jnp.int32),
                pltpu.SMEM(beam_count.shape, jnp.int32),
                pltpu.SemaphoreType.DMA((2 + PIECES,)),
            ],
            compiler_params=limit(16),
            cost_estimate=cost(4 * 10**9, 4 * 10**6),
            name="beams",
        )(in_hbm(centre_offset), in_hbm(counts), in_hbm(operator), spec, within, across, high, low, cosine, sine)
    else:
        live_here = jnp.sum(jnp.where(tiles == mid_index, counts, 0))
        beams = beams_split_time(own, centre_offset, live_here)
        operator_early, operator_late = jnp.split(operator, 2, axis=1)
        first_column = mid_index * operator.shape[1]
        before = jnp.sum(jnp.where(tiles[None, :] < tiles[:, None], counts[None, :], 0), axis=1)
        slot = jnp.arange(CB_DEV, dtype=jnp.int32)
        place = jnp.where(slot[None, :] < counts[:, None], before[:, None] + slot[None, :], -1).reshape(1, rows)
        starts = lax.dynamic_index_in_dim(foot_start, first_column // (FL * DEPTH), 1, keepdims=False)
        position = jnp.arange(live_total, dtype=jnp.int32)
        here = place.reshape(rows, 1) == position[None, :]
        live_starts = jnp.sum(jnp.where(here, starts[:, None], 0), axis=0)
        live_starts = (live_starts + first_column % (FL * DEPTH) // DEPTH).reshape(1, live_total)
    shares = mid_count // P_SIZE
    if shares > 1:
        beams = jnp.repeat(beams, shares, axis=0)
    received = lax.all_to_all(
        beams.reshape(mid_count * CB_DEV, samples), "mid", split_axis=0, concat_axis=0, tiled=True
    )
    partial_image = pl.pallas_call(
        functools.partial(image_stage, scale=1.0 / math.sqrt(FL * P_SIZE), copies=off_count),
        out_shape=jax.ShapeDtypeStruct((mid_count, off_count, CB_DEV, DEPTH), BF16),
        in_specs=[VMEM] * 5,
        out_specs=VMEM,
        compiler_params=limit(24),
        cost_estimate=cost(2 * 10**9, 10**7),
        name="image",
    )(place, live_starts, received, operator_early, operator_late)
    parts = lax.all_to_all(
        partial_image.reshape(mid_count * off_count * CB_DEV, DEPTH),
        ("mid", "off"),
        split_axis=0,
        concat_axis=0,
        tiled=True,
    )
    image = jnp.sum(parts.reshape(mid_count * off_count, CB_DEV, DEPTH).astype(F32), axis=0)
    if sub_count > 1:
        image = lax.psum(image, "sub")
    return image


def solution(mesh):
    return jax.shard_map(
        shards,
        mesh=mesh,
        in_specs=(
            P("off", ("grp", "mid"), "sub"),
            P(("grp", "mid")),
            P("grp", None),
            P("grp"),
            P("sub", "mid"),
        ),
        out_specs=P(("grp", "mid"), None),
        check_vma=False,
    )
```

```python
import functools
import math

import jax
import jax.numpy as jnp
import numpy as np
from jax import lax
from jax.experimental import pallas as pl
from jax.experimental.pallas import tpu as pltpu
from jax.sharding import PartitionSpec as P

NT = 1024
P_SIZE = 16
FL = 16
DEPTH = 256
HALF = 16
CB_DEV = 16
PAIRS = P_SIZE // 2
LANES = 128
PIECES = 4
SHARES = (3, 3)
BF16 = jnp.bfloat16
F32 = jnp.float32


def split_bf16(values):
    high = values.astype(BF16)
    return high, (values - high.astype(values.dtype)).astype(BF16)


def quarter_table():
    phase = np.arange(NT // 4)[:, None] * np.arange(NT // 2)[None, :] % NT
    angle = 2.0 * np.pi / NT * phase
    table = np.concatenate([np.cos(angle), -np.sin(angle)], axis=1) / np.sqrt(NT)
    high = table.astype(BF16)
    return high, (table - high.astype(np.float64)).astype(BF16)


def offset_taper(offsets):
    window = np.exp(-0.5 * (1.5 * np.arange(-HALF, HALF + 1) / HALF) ** 2)
    return np.exp(-0.5 * (1.5 * offsets / HALF) ** 2) / np.sqrt(np.sum(window**2))


def slant_tables():
    offsets = np.arange(HALF + 1)
    slopes = 0.25 * (np.arange(PAIRS) - 0.5 * (P_SIZE - 1))
    theta = (
        2.0 * np.pi / NT * slopes[None, :, None] * offsets[:, None, None] * np.arange(NT // 2)[None, None, :]
    )
    weight = offset_taper(offsets)[:, None, None]
    cosine, sine = weight * np.cos(theta), weight * np.sin(theta)
    shape = (-1, PAIRS, NT // LANES, LANES)
    cosine = np.concatenate([cosine, cosine], axis=2).reshape(shape)
    sine = np.concatenate([sine, -sine], axis=2).reshape(shape)[1:]
    return cosine.astype(np.float32), sine.astype(np.float32)


def store_spectra(traces, high_ref, low_ref, spec_ref):
    quarter = high_ref.shape[0]
    parts = high_ref.shape[1] // LANES
    half = parts // 2
    rows = traces.shape[0]
    folded = jnp.concatenate([traces[:, q * quarter : (q + 1) * quarter] for q in range(4)], axis=0)
    turn = lax.broadcasted_iota(jnp.int32, (rows, LANES), 1) % 4
    odd = turn % 2 == 1
    flip_real = turn >= 2
    flip_imag = (turn == 1) | (turn == 2)
    product = jnp.dot(folded, high_ref[...], preferred_element_type=F32) + jnp.dot(
        folded, low_ref[...], preferred_element_type=F32
    )

    def turned(first, part):
        lanes = slice(part * LANES, (part + 1) * LANES)
        early = product[first * rows : (first + 1) * rows, lanes]
        late = product[(first + 2) * rows : (first + 3) * rows, lanes]
        return early + jnp.where(odd, -late, late)

    for part in range(half):
        real, imag = turned(1, part), turned(1, half + part)
        add_real, add_imag = jnp.where(odd, imag, real), jnp.where(odd, real, imag)
        spec_ref[pl.ds(part, rows, stride=parts), :] = turned(0, part) + jnp.where(
            flip_real, -add_real, add_real
        )
        spec_ref[pl.ds(half + part, rows, stride=parts), :] = turned(0, half + part) + jnp.where(
            flip_imag, -add_imag, add_imag
        )


def live_layout(counts, starts, live):
    padded = starts.shape[1]
    beam = lax.broadcasted_iota(jnp.int32, (1, padded), 1)
    place = jnp.full((1, padded), -1, jnp.int32)
    before = jnp.int32(0)
    for tile in range(padded // CB_DEV):
        slot = beam - tile * CB_DEV
        here = (slot >= 0) & (slot < counts[tile])
        place = jnp.where(here, before + slot, place)
        before = before + counts[tile]
    pick = (lax.broadcasted_iota(jnp.int32, (live, padded), 0) == place).astype(F32).astype(BF16)
    row = lax.broadcasted_iota(jnp.int32, (8, padded), 0)
    digits = jnp.where(row == 0, starts % CB_DEV, jnp.where(row == 1, starts // CB_DEV, 0))
    digits = lax.dot_general(
        digits.astype(F32).astype(BF16), pick, (((1,), (1,)), ((), ())), preferred_element_type=F32
    )
    return place, (digits[0:1] + CB_DEV * digits[1:2]).astype(jnp.int32)


def column_copies(operator_hbm, held_ref, first):
    depth, width = held_ref.shape[0] // PIECES, held_ref.shape[1]
    blocks = [pl.ds(piece * depth, depth) for piece in range(PIECES)]
    return [(operator_hbm.at[rows, pl.ds(first, width)], held_ref.at[rows]) for rows in blocks]


def started(pairs, sems):
    copies = [pltpu.make_async_copy(src, dst, sems.at[i]) for i, (src, dst) in enumerate(pairs)]
    for copy in copies:
        copy.start()
    return copies


def first_stage(
    own_hbm, high_hbm, low_hbm, count_hbm, point_hbm, centre_hbm, cos_hbm, sin_hbm, operator_hbm,
    spec_ref, high_ref, low_ref, cos_ref, sin_ref, early_ref, place_ref, start_ref, count_ref, centre_ref,
    own_ref, point_ref, sems,
):
    pairs = [
        (own_hbm, own_ref), (high_hbm, high_ref), (low_hbm, low_ref), (count_hbm, count_ref),
        (point_hbm, point_ref), (centre_hbm, centre_ref), (cos_hbm, cos_ref), (sin_hbm, sin_ref),
    ]
    copies = started(pairs + column_copies(operator_hbm, early_ref, 0), sems)
    for copy in copies[:5]:
        copy.wait()
    store_spectra(own_ref[...], high_ref, low_ref, spec_ref)
    first_column = lax.axis_index("mid") * operator_hbm.shape[1]
    slope = first_column // (FL * DEPTH)
    rows = lax.broadcasted_iota(jnp.int32, point_ref.shape, 0)
    starts = jnp.sum(jnp.where(rows == slope, point_ref[...], 0), axis=0, keepdims=True)
    place, live_starts = live_layout(count_ref, starts, start_ref.shape[1])
    place_ref[...] = place
    start_ref[...] = live_starts + first_column % (FL * DEPTH) // DEPTH
    for copy in copies[5:]:
        copy.wait()


def beams_stage(
    centre_ref, count_ref, operator_hbm, own_spec_ref, within_ref, across_ref, high_ref, low_ref, cos_ref, sin_ref,
    out_ref, middle_ref, edge_ref, spec_ref, turned_ref, sems, *, first_column,
):
    parts = cos_ref.shape[2]
    copies = started(column_copies(operator_hbm, middle_ref, first_column), sems)
    tile = lax.axis_index("mid")
    at_end = (tile == 0) | (tile == lax.axis_size("mid") - 1)
    within = within_ref[...].astype(F32)
    across = jnp.where(at_end, 0.0, across_ref[...].astype(F32))
    odd_tile = tile % 2 == 1
    above = jnp.where(odd_tile, within, across).astype(BF16)
    below = jnp.where(odd_tile, across, within).astype(BF16)
    edge = HALF * parts
    inner = own_spec_ref.shape[0]
    store_spectra(jnp.concatenate([above, below], axis=0), high_ref, low_ref, edge_ref)
    spec_ref[:edge] = edge_ref[:edge]
    spec_ref[edge : edge + inner] = own_spec_ref[...]
    spec_ref[edge + inner :] = edge_ref[edge:]
    count = count_ref[tile]

    def row(index):
        return spec_ref[pl.ds(pl.multiple_of(index * parts, parts), parts), :]

    def one_beam(beam, carry):
        middle = centre_ref[beam] + HALF
        block = pl.ds(pl.multiple_of(beam * parts, parts), parts)

        @pl.when(beam < count)
        def _():
            centre = row(middle)
            even = [cos_ref[0, j] * centre for j in range(PAIRS)]
            odd_sum = [jnp.zeros_like(centre) for _ in range(PAIRS)]
            for x in range(1, HALF + 1):
                up, down = row(middle + x), row(middle - x)
                both = up + down
                swapped = pltpu.roll(up - down, parts // 2, 0)
                for j in range(PAIRS):
                    even[j] = even[j] + cos_ref[x, j] * both
                    odd_sum[j] = odd_sum[j] + sin_ref[x - 1, j] * swapped
            for j in range(PAIRS):
                turned_ref[j, block, :] = even[j] + odd_sum[j]
                turned_ref[P_SIZE - 1 - j, block, :] = even[j] - odd_sum[j]

        @pl.when(beam >= count)
        def _():
            for j in range(P_SIZE):
                turned_ref[j, block, :] = jnp.zeros((parts, LANES), F32)

        return carry

    lax.fori_loop(0, CB_DEV, one_beam, 0)
    for slope in range(P_SIZE):
        for part in range(parts):
            lanes = slice(part * LANES, (part + 1) * LANES)
            out_ref[slope, :, lanes] = turned_ref[slope, pl.ds(part, CB_DEV, stride=parts), :].astype(BF16)
    for copy in copies:
        copy.wait()


def image_stage(
    place_ref, start_ref, beams_ref, early_ref, middle_ref, operator_hbm, out_ref, late_ref, sems, *, scale, copies
):
    held = [early_ref, middle_ref, late_ref]
    widths = [ref.shape[1] // DEPTH for ref in held]
    arriving = started(column_copies(operator_hbm, late_ref, (widths[0] + widths[1]) * DEPTH), sems)
    live = start_ref.shape[1]
    padded = place_ref.shape[1]
    centres = out_ref.shape[0] * out_ref.shape[2]
    pick = (lax.broadcasted_iota(jnp.int32, (live, padded), 0) == place_ref[...]).astype(F32).astype(BF16)
    chosen = jnp.dot(pick, beams_ref[...], preferred_element_type=F32).astype(BF16)
    point = lax.broadcasted_iota(jnp.int32, (centres, live), 0) - start_ref[...]
    image = jnp.zeros((centres, DEPTH), F32)
    steps = [(ref, column) for ref, width in zip(held, widths) for column in range(width)]
    for step, (operator_ref, column) in enumerate(steps):
        if step == widths[0] + widths[1]:
            for copy in arriving:
                copy.wait()
        columns = slice(column * DEPTH, (column + 1) * DEPTH)
        footprint = jnp.dot(chosen, operator_ref[:, columns], preferred_element_type=F32)
        high, low = split_bf16(footprint)
        hit = (point == step).astype(F32).astype(BF16)
        image = image + jnp.dot(
            jnp.concatenate([hit, hit], axis=1),
            jnp.concatenate([high, low], axis=0),
            preferred_element_type=F32,
        )
    image = (image * scale).astype(BF16)
    tile = out_ref.shape[2]
    for owner in range(out_ref.shape[0]):
        for copy in range(copies):
            out_ref[owner, copy] = image[owner * tile : (owner + 1) * tile]


VMEM = pl.BlockSpec(memory_space=pltpu.VMEM)
SMEM = pl.BlockSpec(memory_space=pltpu.SMEM)
HBM = pl.BlockSpec(memory_space=pltpu.HBM)


def limit(mebibytes):
    return pltpu.CompilerParams(vmem_limit_bytes=mebibytes * 1024 * 1024)


def cost(flops, moved):
    return pl.CostEstimate(flops=flops, bytes_accessed=moved, transcendentals=0)


def in_hbm(array):
    return pltpu.with_memory_space_constraint(jnp.asarray(array), pltpu.HBM)


def shift(cells, axis, step):
    count = lax.axis_size(axis)
    return lax.ppermute(cells, axis, [(i, i + step) for i in range(count) if 0 <= i + step < count])


def beams_split_time(own, centre_offset, live_here):
    high = lax.Precision.HIGHEST
    sub_index = lax.axis_index("sub")
    samples = own.shape[1]
    freq_block = samples // 2
    sample_index = sub_index * samples + jnp.arange(samples, dtype=jnp.int32)[:, None]
    column = jnp.arange(NT, dtype=jnp.int32)[None, :]
    within = column % (2 * freq_block)
    frequency = column // (2 * freq_block) * freq_block + within % freq_block
    angle = 2.0 * math.pi / NT * (sample_index * frequency % NT).astype(F32)
    table = jnp.where(within // freq_block == 1, -jnp.sin(angle), jnp.cos(angle)) / math.sqrt(NT)
    partial_value = jnp.dot(own.astype(F32), table, precision=high)
    spectrum = lax.psum_scatter(partial_value, "sub", scatter_dimension=1, tiled=True)
    above = shift(spectrum[spectrum.shape[0] - HALF :], "mid", 1)
    below = shift(spectrum[:HALF], "mid", -1)
    padded = jnp.concatenate([above, spectrum, below], axis=0)
    windows = padded[centre_offset[:, None] + jnp.arange(2 * HALF + 1, dtype=jnp.int32)[None, :]]
    real, imag = windows[:, :, :freq_block], windows[:, :, freq_block:]
    offsets = np.arange(-HALF, HALF + 1)
    taper = jnp.asarray(offset_taper(offsets).astype(np.float32))[None, :, None]
    slopes = (0.25 * (np.arange(P_SIZE) - 0.5 * (P_SIZE - 1))).astype(np.float32)
    own_freq = (sub_index * freq_block + jnp.arange(freq_block, dtype=jnp.int32)).astype(F32)
    scale = (2.0 * math.pi / NT * slopes[:, None, None] * offsets[None, :, None]).astype(np.float32)
    theta = scale * own_freq[None, None, :]
    cosine, sine = taper * jnp.cos(theta), taper * jnp.sin(theta)
    add = functools.partial(jnp.einsum, "pxf,bxf->pbf", precision=high)
    beams = jnp.concatenate([add(cosine, real) + add(sine, imag), add(cosine, imag) - add(sine, real)], axis=2)
    alive = jnp.arange(CB_DEV, dtype=jnp.int32) < live_here
    return jnp.where(alive[None, :, None], beams, 0.0).astype(BF16)


def shards(traces, centre_offset, foot_start, beam_count, operator):
    mid_count = lax.axis_size("mid")
    off_count = lax.axis_size("off")
    sub_count = lax.axis_size("sub")
    mid_index = lax.axis_index("mid")
    samples = traces.shape[2]
    own = traces[0]
    counts = beam_count.astype(jnp.int32)
    tiles = jnp.arange(mid_count, dtype=jnp.int32)
    rows = mid_count * CB_DEV
    live_total = rows // 2
    steps = operator.shape[1] // DEPTH
    early_width, middle_width = (steps * share // 8 * DEPTH for share in SHARES)
    if sub_count == 1:
        odd_tile = mid_index % 2 == 1
        head, tail = own[:HALF], own[own.shape[0] - HALF :]
        ends = [(0, 0), (mid_count - 1, mid_count - 1)]
        inner_pairs = [(i, i - 1 if i % 2 == 0 else i + 1) for i in range(1, mid_count - 1)]
        within = lax.ppermute(jnp.where(odd_tile, head, tail), "mid", [(i, i ^ 1) for i in range(mid_count)])
        across = lax.ppermute(jnp.where(odd_tile, tail, head), "mid", ends + inner_pairs)
        tables = quarter_table() + slant_tables()
        parts = samples // LANES
        inner = own.shape[0] * parts
        edge = 2 * HALF * parts
        spec, high, low, cosine, sine, early, place, live_starts, count_held, centre_held = pl.pallas_call(
            first_stage,
            out_shape=[pltpu.VMEM((inner, LANES), F32)]
            + [pltpu.VMEM(t.shape, t.dtype) for t in tables]
            + [pltpu.VMEM((samples, early_width), BF16)]
            + [pltpu.VMEM((1, n), jnp.int32) for n in (rows, live_total)]
            + [pltpu.SMEM(t.shape, jnp.int32) for t in (counts, centre_offset)],
            in_specs=[HBM] * 9,
            out_specs=[VMEM] * 8 + [SMEM] * 2,
            scratch_shapes=[
                pltpu.VMEM(own.shape, BF16),
                pltpu.VMEM((P_SIZE, rows), jnp.int32),
                pltpu.SemaphoreType.DMA((8 + PIECES,)),
            ],
            compiler_params=limit(16),
            cost_estimate=cost(4 * 10**9, 10**7),
            name="first",
        )(*(in_hbm(t) for t in (own,) + tables[:2] + (counts, foot_start.T, centre_offset) + tables[2:] + (operator,)))
        beams, middle = pl.pallas_call(
            functools.partial(beams_stage, first_column=early_width),
            out_shape=[pltpu.VMEM((P_SIZE, CB_DEV, samples), BF16), pltpu.VMEM((samples, middle_width), BF16)],
            in_specs=[SMEM, SMEM, HBM] + [VMEM] * 7,
            out_specs=[VMEM] * 2,
            scratch_shapes=[
                pltpu.VMEM((edge, LANES), F32),
                pltpu.VMEM((edge + inner, LANES), F32),
                pltpu.VMEM((P_SIZE, CB_DEV * parts, LANES), F32),
                pltpu.SemaphoreType.DMA((PIECES,)),
            ],
            compiler_params=limit(16),
            cost_estimate=cost(4 * 10**9, 4 * 10**6),
            name="beams",
        )(centre_held, count_held, in_hbm(operator), spec, within, across, high, low, cosine, sine)
    else:
        live_here = jnp.sum(jnp.where(tiles == mid_index, counts, 0))
        beams = beams_split_time(own, centre_offset, live_here)
        early, middle = operator[:, :early_width], operator[:, early_width : early_width + middle_width]
        first_column = mid_index * operator.shape[1]
        before = jnp.sum(jnp.where(tiles[None, :] < tiles[:, None], counts[None, :], 0), axis=1)
        slot = jnp.arange(CB_DEV, dtype=jnp.int32)
        place = jnp.where(slot[None, :] < counts[:, None], before[:, None] + slot[None, :], -1).reshape(1, rows)
        starts = lax.dynamic_index_in_dim(foot_start, first_column // (FL * DEPTH), 1, keepdims=False)
        position = jnp.arange(live_total, dtype=jnp.int32)
        here = place.reshape(rows, 1) == position[None, :]
        live_starts = jnp.sum(jnp.where(here, starts[:, None], 0), axis=0)
        live_starts = (live_starts + first_column % (FL * DEPTH) // DEPTH).reshape(1, live_total)
    shares = mid_count // P_SIZE
    if shares > 1:
        beams = jnp.repeat(beams, shares, axis=0)
    received = lax.all_to_all(
        beams.reshape(mid_count * CB_DEV, samples), "mid", split_axis=0, concat_axis=0, tiled=True
    )
    partial_image = pl.pallas_call(
        functools.partial(image_stage, scale=1.0 / math.sqrt(FL * P_SIZE), copies=off_count),
        out_shape=jax.ShapeDtypeStruct((mid_count, off_count, CB_DEV, DEPTH), BF16),
        in_specs=[VMEM] * 5 + [HBM],
        out_specs=VMEM,
        scratch_shapes=[
            pltpu.VMEM((samples, operator.shape[1] - early_width - middle_width), BF16),
            pltpu.SemaphoreType.DMA((PIECES,)),
        ],
        compiler_params=limit(24),
        cost_estimate=cost(2 * 10**9, 10**7),
        name="image",
    )(place, live_starts, received, early, middle, in_hbm(operator))
    parts = lax.all_to_all(
        partial_image.reshape(mid_count * off_count * CB_DEV, DEPTH),
        ("mid", "off"),
        split_axis=0,
        concat_axis=0,
        tiled=True,
    )
    image = jnp.sum(parts.reshape(mid_count * off_count, CB_DEV, DEPTH).astype(F32), axis=0)
    if sub_count > 1:
        image = lax.psum(image, "sub")
    return image


def solution(mesh):
    return jax.shard_map(
        shards,
        mesh=mesh,
        in_specs=(
            P("off", ("grp", "mid"), "sub"),
            P(("grp", "mid")),
            P("grp", None),
            P("grp"),
            P("sub", "mid"),
        ),
        out_specs=P(("grp", "mid"), None),
        check_vma=False,
    )
```

```python
import functools
import math

import jax
import jax.numpy as jnp
import numpy as np
from jax import lax
from jax.experimental import pallas as pl
from jax.experimental.pallas import tpu as pltpu
from jax.sharding import PartitionSpec as P

NT = 1024
P_SIZE = 16
FL = 16
DEPTH = 256
HALF = 16
CB_DEV = 16
PAIRS = P_SIZE // 2
LANES = 128
PIECES = 4
SHARES = (3, 3)
BLOCKS = (2, 0, 3, 1)
BF16 = jnp.bfloat16
F32 = jnp.float32


def split_bf16(values):
    high = values.astype(BF16)
    return high, (values - high.astype(values.dtype)).astype(BF16)


def quarter_table():
    phase = np.arange(NT // 4)[:, None] * np.arange(NT // 2)[None, :] % NT
    angle = 2.0 * np.pi / NT * phase
    table = np.concatenate([np.cos(angle), -np.sin(angle)], axis=1) / np.sqrt(NT)
    high = table.astype(BF16)
    return high, (table - high.astype(np.float64)).astype(BF16)


def offset_taper(offsets):
    window = np.exp(-0.5 * (1.5 * np.arange(-HALF, HALF + 1) / HALF) ** 2)
    return np.exp(-0.5 * (1.5 * offsets / HALF) ** 2) / np.sqrt(np.sum(window**2))


def slant_tables():
    offsets = np.arange(HALF + 1)
    slopes = 0.25 * (np.arange(PAIRS) - 0.5 * (P_SIZE - 1))
    theta = (
        2.0 * np.pi / NT * slopes[None, :, None] * offsets[:, None, None] * np.arange(NT // 2)[None, None, :]
    )
    weight = offset_taper(offsets)[:, None, None]
    cosine, sine = weight * np.cos(theta), weight * np.sin(theta)
    shape = (-1, PAIRS, NT // LANES, LANES)
    cosine = np.concatenate([cosine, cosine], axis=2).reshape(shape)
    sine = np.concatenate([sine, -sine], axis=2).reshape(shape)[1:]
    return cosine.astype(np.float32), sine.astype(np.float32)


def store_spectra(traces, high_ref, low_ref, spec_ref):
    quarter = high_ref.shape[0]
    parts = high_ref.shape[1] // LANES
    half = parts // 2
    rows = traces.shape[0]
    folded = jnp.concatenate([traces[:, q * quarter : (q + 1) * quarter] for q in range(4)], axis=0)
    turn = lax.broadcasted_iota(jnp.int32, (rows, LANES), 1) % 4
    odd = turn % 2 == 1
    flip_real = turn >= 2
    flip_imag = (turn == 1) | (turn == 2)
    product = jnp.dot(folded, high_ref[...], preferred_element_type=F32) + jnp.dot(
        folded, low_ref[...], preferred_element_type=F32
    )

    def turned(first, part):
        lanes = slice(part * LANES, (part + 1) * LANES)
        early = product[first * rows : (first + 1) * rows, lanes]
        late = product[(first + 2) * rows : (first + 3) * rows, lanes]
        return early + jnp.where(odd, -late, late)

    for part in range(half):
        real, imag = turned(1, part), turned(1, half + part)
        add_real, add_imag = jnp.where(odd, imag, real), jnp.where(odd, real, imag)
        spec_ref[pl.ds(part, rows, stride=parts), :] = turned(0, part) + jnp.where(
            flip_real, -add_real, add_real
        )
        spec_ref[pl.ds(half + part, rows, stride=parts), :] = turned(0, half + part) + jnp.where(
            flip_imag, -add_imag, add_imag
        )


def travel_order(count):
    block = count // len(BLOCKS)
    return [first * block + step for step in range(block) for first in BLOCKS]


def live_layout(counts, starts, live):
    padded = starts.shape[1]
    tiles = padded // CB_DEV
    order = travel_order(tiles)
    beam = lax.broadcasted_iota(jnp.int32, (1, padded), 1)
    place = jnp.full((1, padded), -1, jnp.int32)
    own_place = place
    before = jnp.int32(0)
    for tile in range(tiles):
        own_slot = beam - tile * CB_DEV
        slot = beam - order.index(tile) * CB_DEV
        own_place = jnp.where((own_slot >= 0) & (own_slot < counts[tile]), before + own_slot, own_place)
        place = jnp.where((slot >= 0) & (slot < counts[tile]), before + slot, place)
        before = before + counts[tile]
    pick = (lax.broadcasted_iota(jnp.int32, (live, padded), 0) == own_place).astype(F32).astype(BF16)
    row = lax.broadcasted_iota(jnp.int32, (8, padded), 0)
    digits = jnp.where(row == 0, starts % CB_DEV, jnp.where(row == 1, starts // CB_DEV, 0))
    digits = lax.dot_general(
        digits.astype(F32).astype(BF16), pick, (((1,), (1,)), ((), ())), preferred_element_type=F32
    )
    return place, (digits[0:1] + CB_DEV * digits[1:2]).astype(jnp.int32)


def column_copies(operator_hbm, held_ref, first):
    depth, width = held_ref.shape[0] // PIECES, held_ref.shape[1]
    blocks = [pl.ds(piece * depth, depth) for piece in range(PIECES)]
    return [(operator_hbm.at[rows, pl.ds(first, width)], held_ref.at[rows]) for rows in blocks]


def started(pairs, sems):
    copies = [pltpu.make_async_copy(src, dst, sems.at[i]) for i, (src, dst) in enumerate(pairs)]
    for copy in copies:
        copy.start()
    return copies


def first_stage(
    own_hbm, high_hbm, low_hbm, count_hbm, point_hbm, centre_hbm, cos_hbm, sin_hbm, operator_hbm,
    spec_ref, high_ref, low_ref, cos_ref, sin_ref, early_ref, place_ref, start_ref, count_ref, centre_ref,
    own_ref, point_ref, sems,
):
    pairs = [
        (own_hbm, own_ref), (high_hbm, high_ref), (low_hbm, low_ref), (count_hbm, count_ref),
        (point_hbm, point_ref), (centre_hbm, centre_ref), (cos_hbm, cos_ref), (sin_hbm, sin_ref),
    ]
    copies = started(pairs + column_copies(operator_hbm, early_ref, 0), sems)
    for copy in copies[:5]:
        copy.wait()
    store_spectra(own_ref[...], high_ref, low_ref, spec_ref)
    first_column = lax.axis_index("mid") * operator_hbm.shape[1]
    slope = first_column // (FL * DEPTH)
    rows = lax.broadcasted_iota(jnp.int32, point_ref.shape, 0)
    starts = jnp.sum(jnp.where(rows == slope, point_ref[...], 0), axis=0, keepdims=True)
    place, live_starts = live_layout(count_ref, starts, start_ref.shape[1])
    place_ref[...] = place
    start_ref[...] = live_starts + first_column % (FL * DEPTH) // DEPTH
    for copy in copies[5:]:
        copy.wait()


def beams_stage(
    centre_ref, count_ref, operator_hbm, own_spec_ref, within_ref, across_ref, high_ref, low_ref, cos_ref, sin_ref,
    out_ref, middle_ref, edge_ref, spec_ref, turned_ref, sems, *, first_column,
):
    parts = cos_ref.shape[2]
    copies = started(column_copies(operator_hbm, middle_ref, first_column), sems)
    tile = lax.axis_index("mid")
    at_end = (tile == 0) | (tile == lax.axis_size("mid") - 1)
    within = within_ref[...].astype(F32)
    across = jnp.where(at_end, 0.0, across_ref[...].astype(F32))
    odd_tile = tile % 2 == 1
    above = jnp.where(odd_tile, within, across).astype(BF16)
    below = jnp.where(odd_tile, across, within).astype(BF16)
    edge = HALF * parts
    inner = own_spec_ref.shape[0]
    store_spectra(jnp.concatenate([above, below], axis=0), high_ref, low_ref, edge_ref)
    spec_ref[:edge] = edge_ref[:edge]
    spec_ref[edge : edge + inner] = own_spec_ref[...]
    spec_ref[edge + inner :] = edge_ref[edge:]
    count = count_ref[tile]

    def row(index):
        return spec_ref[pl.ds(pl.multiple_of(index * parts, parts), parts), :]

    def one_beam(beam, carry):
        middle = centre_ref[beam] + HALF
        block = pl.ds(pl.multiple_of(beam * parts, parts), parts)

        @pl.when(beam < count)
        def _():
            centre = row(middle)
            even = [cos_ref[0, j] * centre for j in range(PAIRS)]
            odd_sum = [jnp.zeros_like(centre) for _ in range(PAIRS)]
            for x in range(1, HALF + 1):
                up, down = row(middle + x), row(middle - x)
                both = up + down
                swapped = pltpu.roll(up - down, parts // 2, 0)
                for j in range(PAIRS):
                    even[j] = even[j] + cos_ref[x, j] * both
                    odd_sum[j] = odd_sum[j] + sin_ref[x - 1, j] * swapped
            for j in range(PAIRS):
                turned_ref[j, block, :] = even[j] + odd_sum[j]
                turned_ref[P_SIZE - 1 - j, block, :] = even[j] - odd_sum[j]

        @pl.when(beam >= count)
        def _():
            for j in range(P_SIZE):
                turned_ref[j, block, :] = jnp.zeros((parts, LANES), F32)

        return carry

    lax.fori_loop(0, CB_DEV, one_beam, 0)
    destinations = out_ref.shape[0]
    for position, tile_index in enumerate(travel_order(destinations)):
        slope = tile_index // (destinations // P_SIZE)
        for part in range(parts):
            lanes = slice(part * LANES, (part + 1) * LANES)
            out_ref[position, :, lanes] = turned_ref[slope, pl.ds(part, CB_DEV, stride=parts), :].astype(BF16)
    for copy in copies:
        copy.wait()


def image_stage(
    place_ref, start_ref, beams_ref, early_ref, middle_ref, operator_hbm, out_ref, late_ref, sems, *, scale, copies
):
    held = [early_ref, middle_ref, late_ref]
    widths = [ref.shape[1] // DEPTH for ref in held]
    arriving = started(column_copies(operator_hbm, late_ref, (widths[0] + widths[1]) * DEPTH), sems)
    live = start_ref.shape[1]
    padded = place_ref.shape[1]
    centres = out_ref.shape[0] * out_ref.shape[2]
    pick = (lax.broadcasted_iota(jnp.int32, (live, padded), 0) == place_ref[...]).astype(F32).astype(BF16)
    chosen = jnp.dot(pick, beams_ref[...], preferred_element_type=F32).astype(BF16)
    point = lax.broadcasted_iota(jnp.int32, (centres, live), 0) - start_ref[...]
    image = jnp.zeros((centres, DEPTH), F32)
    steps = [(ref, column) for ref, width in zip(held, widths) for column in range(width)]
    for step, (operator_ref, column) in enumerate(steps):
        if step == widths[0] + widths[1]:
            for copy in arriving:
                copy.wait()
        columns = slice(column * DEPTH, (column + 1) * DEPTH)
        footprint = jnp.dot(chosen, operator_ref[:, columns], preferred_element_type=F32)
        high, low = split_bf16(footprint)
        hit = (point == step).astype(F32).astype(BF16)
        image = image + jnp.dot(
            jnp.concatenate([hit, hit], axis=1),
            jnp.concatenate([high, low], axis=0),
            preferred_element_type=F32,
        )
    image = (image * scale).astype(BF16)
    tile = out_ref.shape[2]
    for owner in range(out_ref.shape[0]):
        for copy in range(copies):
            out_ref[owner, copy] = image[owner * tile : (owner + 1) * tile]


VMEM = pl.BlockSpec(memory_space=pltpu.VMEM)
SMEM = pl.BlockSpec(memory_space=pltpu.SMEM)
HBM = pl.BlockSpec(memory_space=pltpu.HBM)


def limit(mebibytes):
    return pltpu.CompilerParams(vmem_limit_bytes=mebibytes * 1024 * 1024)


def cost(flops, moved):
    return pl.CostEstimate(flops=flops, bytes_accessed=moved, transcendentals=0)


def in_hbm(array):
    return pltpu.with_memory_space_constraint(jnp.asarray(array), pltpu.HBM)


def shift(cells, axis, step):
    count = lax.axis_size(axis)
    return lax.ppermute(cells, axis, [(i, i + step) for i in range(count) if 0 <= i + step < count])


def beams_split_time(own, centre_offset, live_here):
    high = lax.Precision.HIGHEST
    sub_index = lax.axis_index("sub")
    samples = own.shape[1]
    freq_block = samples // 2
    sample_index = sub_index * samples + jnp.arange(samples, dtype=jnp.int32)[:, None]
    column = jnp.arange(NT, dtype=jnp.int32)[None, :]
    within = column % (2 * freq_block)
    frequency = column // (2 * freq_block) * freq_block + within % freq_block
    angle = 2.0 * math.pi / NT * (sample_index * frequency % NT).astype(F32)
    table = jnp.where(within // freq_block == 1, -jnp.sin(angle), jnp.cos(angle)) / math.sqrt(NT)
    partial_value = jnp.dot(own.astype(F32), table, precision=high)
    spectrum = lax.psum_scatter(partial_value, "sub", scatter_dimension=1, tiled=True)
    above = shift(spectrum[spectrum.shape[0] - HALF :], "mid", 1)
    below = shift(spectrum[:HALF], "mid", -1)
    padded = jnp.concatenate([above, spectrum, below], axis=0)
    windows = padded[centre_offset[:, None] + jnp.arange(2 * HALF + 1, dtype=jnp.int32)[None, :]]
    real, imag = windows[:, :, :freq_block], windows[:, :, freq_block:]
    offsets = np.arange(-HALF, HALF + 1)
    taper = jnp.asarray(offset_taper(offsets).astype(np.float32))[None, :, None]
    slopes = (0.25 * (np.arange(P_SIZE) - 0.5 * (P_SIZE - 1))).astype(np.float32)
    own_freq = (sub_index * freq_block + jnp.arange(freq_block, dtype=jnp.int32)).astype(F32)
    scale = (2.0 * math.pi / NT * slopes[:, None, None] * offsets[None, :, None]).astype(np.float32)
    theta = scale * own_freq[None, None, :]
    cosine, sine = taper * jnp.cos(theta), taper * jnp.sin(theta)
    add = functools.partial(jnp.einsum, "pxf,bxf->pbf", precision=high)
    beams = jnp.concatenate([add(cosine, real) + add(sine, imag), add(cosine, imag) - add(sine, real)], axis=2)
    alive = jnp.arange(CB_DEV, dtype=jnp.int32) < live_here
    return jnp.where(alive[None, :, None], beams, 0.0).astype(BF16)


def shards(traces, centre_offset, foot_start, beam_count, operator):
    mid_count = lax.axis_size("mid")
    off_count = lax.axis_size("off")
    sub_count = lax.axis_size("sub")
    mid_index = lax.axis_index("mid")
    samples = traces.shape[2]
    own = traces[0]
    counts = beam_count.astype(jnp.int32)
    tiles = jnp.arange(mid_count, dtype=jnp.int32)
    rows = mid_count * CB_DEV
    live_total = rows // 2
    steps = operator.shape[1] // DEPTH
    early_width, middle_width = (steps * share // 8 * DEPTH for share in SHARES)
    if sub_count == 1:
        odd_tile = mid_index % 2 == 1
        head, tail = own[:HALF], own[own.shape[0] - HALF :]
        ends = [(0, 0), (mid_count - 1, mid_count - 1)]
        inner_pairs = [(i, i - 1 if i % 2 == 0 else i + 1) for i in range(1, mid_count - 1)]
        within = lax.ppermute(jnp.where(odd_tile, head, tail), "mid", [(i, i ^ 1) for i in range(mid_count)])
        across = lax.ppermute(jnp.where(odd_tile, tail, head), "mid", ends + inner_pairs)
        tables = quarter_table() + slant_tables()
        parts = samples // LANES
        inner = own.shape[0] * parts
        edge = 2 * HALF * parts
        spec, high, low, cosine, sine, early, place, live_starts, count_held, centre_held = pl.pallas_call(
            first_stage,
            out_shape=[pltpu.VMEM((inner, LANES), F32)]
            + [pltpu.VMEM(t.shape, t.dtype) for t in tables]
            + [pltpu.VMEM((samples, early_width), BF16)]
            + [pltpu.VMEM((1, n), jnp.int32) for n in (rows, live_total)]
            + [pltpu.SMEM(t.shape, jnp.int32) for t in (counts, centre_offset)],
            in_specs=[HBM] * 9,
            out_specs=[VMEM] * 8 + [SMEM] * 2,
            scratch_shapes=[
                pltpu.VMEM(own.shape, BF16),
                pltpu.VMEM((P_SIZE, rows), jnp.int32),
                pltpu.SemaphoreType.DMA((8 + PIECES,)),
            ],
            compiler_params=limit(16),
            cost_estimate=cost(4 * 10**9, 10**7),
            name="first",
        )(*(in_hbm(t) for t in (own,) + tables[:2] + (counts, foot_start.T, centre_offset) + tables[2:] + (operator,)))
        beams, middle = pl.pallas_call(
            functools.partial(beams_stage, first_column=early_width),
            out_shape=[pltpu.VMEM((mid_count, CB_DEV, samples), BF16), pltpu.VMEM((samples, middle_width), BF16)],
            in_specs=[SMEM, SMEM, HBM] + [VMEM] * 7,
            out_specs=[VMEM] * 2,
            scratch_shapes=[
                pltpu.VMEM((edge, LANES), F32),
                pltpu.VMEM((edge + inner, LANES), F32),
                pltpu.VMEM((P_SIZE, CB_DEV * parts, LANES), F32),
                pltpu.SemaphoreType.DMA((PIECES,)),
            ],
            compiler_params=limit(16),
            cost_estimate=cost(4 * 10**9, 4 * 10**6),
            name="beams",
        )(centre_held, count_held, in_hbm(operator), spec, within, across, high, low, cosine, sine)
    else:
        live_here = jnp.sum(jnp.where(tiles == mid_index, counts, 0))
        order = np.array(travel_order(mid_count))
        beams = beams_split_time(own, centre_offset, live_here)[order // (mid_count // P_SIZE)]
        early, middle = operator[:, :early_width], operator[:, early_width : early_width + middle_width]
        first_column = mid_index * operator.shape[1]
        before = jnp.sum(jnp.where(tiles[None, :] < tiles[:, None], counts[None, :], 0), axis=1)
        slot = jnp.arange(CB_DEV, dtype=jnp.int32)
        place = jnp.where(slot[None, :] < counts[:, None], before[:, None] + slot[None, :], -1).reshape(1, rows)
        starts = lax.dynamic_index_in_dim(foot_start, first_column // (FL * DEPTH), 1, keepdims=False)
        position = jnp.arange(live_total, dtype=jnp.int32)
        here = place.reshape(rows, 1) == position[None, :]
        live_starts = jnp.sum(jnp.where(here, starts[:, None], 0), axis=0)
        live_starts = (live_starts + first_column % (FL * DEPTH) // DEPTH).reshape(1, live_total)
        place = place.reshape(mid_count, CB_DEV)[order].reshape(1, rows)
    received = lax.all_to_all(
        beams.reshape(rows, samples),
        "mid",
        split_axis=0,
        concat_axis=0,
        tiled=True,
        axis_index_groups=[travel_order(mid_count)],
    )
    partial_image = pl.pallas_call(
        functools.partial(image_stage, scale=1.0 / math.sqrt(FL * P_SIZE), copies=off_count),
        out_shape=jax.ShapeDtypeStruct((mid_count, off_count, CB_DEV, DEPTH), BF16),
        in_specs=[VMEM] * 5 + [HBM],
        out_specs=VMEM,
        scratch_shapes=[
            pltpu.VMEM((samples, operator.shape[1] - early_width - middle_width), BF16),
            pltpu.SemaphoreType.DMA((PIECES,)),
        ],
        compiler_params=limit(24),
        cost_estimate=cost(2 * 10**9, 10**7),
        name="image",
    )(place, live_starts, received, early, middle, in_hbm(operator))
    parts = lax.all_to_all(
        partial_image.reshape(mid_count * off_count * CB_DEV, DEPTH),
        ("mid", "off"),
        split_axis=0,
        concat_axis=0,
        tiled=True,
    )
    image = jnp.sum(parts.reshape(mid_count * off_count, CB_DEV, DEPTH).astype(F32), axis=0)
    if sub_count > 1:
        image = lax.psum(image, "sub")
    return image


def solution(mesh):
    return jax.shard_map(
        shards,
        mesh=mesh,
        in_specs=(
            P("off", ("grp", "mid"), "sub"),
            P(("grp", "mid")),
            P("grp", None),
            P("grp"),
            P("sub", "mid"),
        ),
        out_specs=P(("grp", "mid"), None),
        check_vma=False,
    )
```

```python
import functools
import math

import jax
import jax.numpy as jnp
import numpy as np
from jax import lax
from jax.experimental import pallas as pl
from jax.experimental.pallas import tpu as pltpu
from jax.sharding import PartitionSpec as P

NT = 1024
P_SIZE = 16
FL = 16
DEPTH = 256
HALF = 16
CB_DEV = 16
PAIRS = P_SIZE // 2
LANES = 128
PIECES = 4
SHARES = (3, 3)
BLOCKS = (1, 3, 0, 2)
BF16 = jnp.bfloat16
F32 = jnp.float32


def split_bf16(values):
    high = values.astype(BF16)
    return high, (values - high.astype(values.dtype)).astype(BF16)


def quarter_table():
    phase = np.arange(NT // 4)[:, None] * np.arange(NT // 2)[None, :] % NT
    angle = 2.0 * np.pi / NT * phase
    table = np.concatenate([np.cos(angle), -np.sin(angle)], axis=1) / np.sqrt(NT)
    high = table.astype(BF16)
    return high, (table - high.astype(np.float64)).astype(BF16)


def offset_taper(offsets):
    window = np.exp(-0.5 * (1.5 * np.arange(-HALF, HALF + 1) / HALF) ** 2)
    return np.exp(-0.5 * (1.5 * offsets / HALF) ** 2) / np.sqrt(np.sum(window**2))


def slant_tables():
    offsets = np.arange(HALF + 1)
    slopes = 0.25 * (np.arange(PAIRS) - 0.5 * (P_SIZE - 1))
    theta = (
        2.0 * np.pi / NT * slopes[None, :, None] * offsets[:, None, None] * np.arange(NT // 2)[None, None, :]
    )
    weight = offset_taper(offsets)[:, None, None]
    cosine, sine = weight * np.cos(theta), weight * np.sin(theta)
    shape = (-1, PAIRS, NT // LANES, LANES)
    cosine = np.concatenate([cosine, cosine], axis=2).reshape(shape)
    sine = np.concatenate([sine, -sine], axis=2).reshape(shape)[1:]
    return cosine.astype(np.float32), sine.astype(np.float32)


def store_spectra(traces, high_ref, low_ref, spec_ref):
    quarter = high_ref.shape[0]
    parts = high_ref.shape[1] // LANES
    half = parts // 2
    rows = traces.shape[0]
    folded = jnp.concatenate([traces[:, q * quarter : (q + 1) * quarter] for q in range(4)], axis=0)
    turn = lax.broadcasted_iota(jnp.int32, (rows, LANES), 1) % 4
    odd = turn % 2 == 1
    flip_real = turn >= 2
    flip_imag = (turn == 1) | (turn == 2)
    product = jnp.dot(folded, high_ref[...], preferred_element_type=F32) + jnp.dot(
        folded, low_ref[...], preferred_element_type=F32
    )

    def turned(first, part):
        lanes = slice(part * LANES, (part + 1) * LANES)
        early = product[first * rows : (first + 1) * rows, lanes]
        late = product[(first + 2) * rows : (first + 3) * rows, lanes]
        return early + jnp.where(odd, -late, late)

    for part in range(half):
        real, imag = turned(1, part), turned(1, half + part)
        add_real, add_imag = jnp.where(odd, imag, real), jnp.where(odd, real, imag)
        spec_ref[pl.ds(part, rows, stride=parts), :] = turned(0, part) + jnp.where(
            flip_real, -add_real, add_real
        )
        spec_ref[pl.ds(half + part, rows, stride=parts), :] = turned(0, half + part) + jnp.where(
            flip_imag, -add_imag, add_imag
        )


def travel_order(count):
    block = count // len(BLOCKS)
    return [first * block + step for step in range(block) for first in BLOCKS]


def live_layout(counts, starts, live):
    padded = starts.shape[1]
    tiles = padded // CB_DEV
    order = travel_order(tiles)
    beam = lax.broadcasted_iota(jnp.int32, (1, padded), 1)
    place = jnp.full((1, padded), -1, jnp.int32)
    own_place = place
    before = jnp.int32(0)
    for tile in range(tiles):
        own_slot = beam - tile * CB_DEV
        slot = beam - order.index(tile) * CB_DEV
        own_place = jnp.where((own_slot >= 0) & (own_slot < counts[tile]), before + own_slot, own_place)
        place = jnp.where((slot >= 0) & (slot < counts[tile]), before + slot, place)
        before = before + counts[tile]
    pick = (lax.broadcasted_iota(jnp.int32, (live, padded), 0) == own_place).astype(F32).astype(BF16)
    row = lax.broadcasted_iota(jnp.int32, (8, padded), 0)
    digits = jnp.where(row == 0, starts % CB_DEV, jnp.where(row == 1, starts // CB_DEV, 0))
    digits = lax.dot_general(
        digits.astype(F32).astype(BF16), pick, (((1,), (1,)), ((), ())), preferred_element_type=F32
    )
    return place, (digits[0:1] + CB_DEV * digits[1:2]).astype(jnp.int32)


def column_copies(operator_hbm, held_ref, first):
    depth, width = held_ref.shape[0] // PIECES, held_ref.shape[1]
    blocks = [pl.ds(piece * depth, depth) for piece in range(PIECES)]
    return [(operator_hbm.at[rows, pl.ds(first, width)], held_ref.at[rows]) for rows in blocks]


def started(pairs, sems):
    copies = [pltpu.make_async_copy(src, dst, sems.at[i]) for i, (src, dst) in enumerate(pairs)]
    for copy in copies:
        copy.start()
    return copies


def first_stage(
    own_hbm, high_hbm, low_hbm, count_hbm, point_hbm, centre_hbm, cos_hbm, sin_hbm, operator_hbm,
    spec_ref, high_ref, low_ref, cos_ref, sin_ref, early_ref, place_ref, start_ref, count_ref, centre_ref,
    own_ref, point_ref, sems,
):
    pairs = [
        (own_hbm, own_ref), (high_hbm, high_ref), (low_hbm, low_ref), (count_hbm, count_ref),
        (point_hbm, point_ref), (centre_hbm, centre_ref), (cos_hbm, cos_ref), (sin_hbm, sin_ref),
    ]
    copies = started(pairs + column_copies(operator_hbm, early_ref, 0), sems)
    for copy in copies[:5]:
        copy.wait()
    store_spectra(own_ref[...], high_ref, low_ref, spec_ref)
    first_column = lax.axis_index("mid") * operator_hbm.shape[1]
    slope = first_column // (FL * DEPTH)
    rows = lax.broadcasted_iota(jnp.int32, point_ref.shape, 0)
    starts = jnp.sum(jnp.where(rows == slope, point_ref[...], 0), axis=0, keepdims=True)
    place, live_starts = live_layout(count_ref, starts, start_ref.shape[1])
    place_ref[...] = place
    start_ref[...] = live_starts + first_column % (FL * DEPTH) // DEPTH
    for copy in copies[5:]:
        copy.wait()


def beams_stage(
    centre_ref, count_ref, operator_hbm, own_spec_ref, within_ref, across_ref, high_ref, low_ref, cos_ref, sin_ref,
    out_ref, middle_ref, edge_ref, spec_ref, turned_ref, sems, *, first_column,
):
    parts = cos_ref.shape[2]
    copies = started(column_copies(operator_hbm, middle_ref, first_column), sems)
    tile = lax.axis_index("mid")
    at_end = (tile == 0) | (tile == lax.axis_size("mid") - 1)
    within = within_ref[...].astype(F32)
    across = jnp.where(at_end, 0.0, across_ref[...].astype(F32))
    odd_tile = tile % 2 == 1
    above = jnp.where(odd_tile, within, across).astype(BF16)
    below = jnp.where(odd_tile, across, within).astype(BF16)
    edge = HALF * parts
    inner = own_spec_ref.shape[0]
    store_spectra(jnp.concatenate([above, below], axis=0), high_ref, low_ref, edge_ref)
    spec_ref[:edge] = edge_ref[:edge]
    spec_ref[edge : edge + inner] = own_spec_ref[...]
    spec_ref[edge + inner :] = edge_ref[edge:]
    count = count_ref[tile]

    def row(index):
        return spec_ref[pl.ds(pl.multiple_of(index * parts, parts), parts), :]

    def one_beam(beam, carry):
        middle = centre_ref[beam] + HALF
        block = pl.ds(pl.multiple_of(beam * parts, parts), parts)

        @pl.when(beam < count)
        def _():
            centre = row(middle)
            even = [cos_ref[0, j] * centre for j in range(PAIRS)]
            odd_sum = [jnp.zeros_like(centre) for _ in range(PAIRS)]
            for x in range(1, HALF + 1):
                up, down = row(middle + x), row(middle - x)
                both = up + down
                swapped = pltpu.roll(up - down, parts // 2, 0)
                for j in range(PAIRS):
                    even[j] = even[j] + cos_ref[x, j] * both
                    odd_sum[j] = odd_sum[j] + sin_ref[x - 1, j] * swapped
            for j in range(PAIRS):
                turned_ref[j, block, :] = even[j] + odd_sum[j]
                turned_ref[P_SIZE - 1 - j, block, :] = even[j] - odd_sum[j]

        @pl.when(beam >= count)
        def _():
            for j in range(P_SIZE):
                turned_ref[j, block, :] = jnp.zeros((parts, LANES), F32)

        return carry

    lax.fori_loop(0, CB_DEV, one_beam, 0)
    destinations = out_ref.shape[0]
    for position, tile_index in enumerate(travel_order(destinations)):
        slope = tile_index // (destinations // P_SIZE)
        for part in range(parts):
            lanes = slice(part * LANES, (part + 1) * LANES)
            out_ref[position, :, lanes] = turned_ref[slope, pl.ds(part, CB_DEV, stride=parts), :].astype(BF16)
    for copy in copies:
        copy.wait()


def image_stage(
    place_ref, start_ref, beams_ref, early_ref, middle_ref, operator_hbm, out_ref, late_ref, sems, *, scale, copies
):
    held = [early_ref, middle_ref, late_ref]
    widths = [ref.shape[1] // DEPTH for ref in held]
    arriving = started(column_copies(operator_hbm, late_ref, (widths[0] + widths[1]) * DEPTH), sems)
    live = start_ref.shape[1]
    padded = place_ref.shape[1]
    centres = out_ref.shape[0] * out_ref.shape[2]
    pick = (lax.broadcasted_iota(jnp.int32, (live, padded), 0) == place_ref[...]).astype(F32).astype(BF16)
    chosen = jnp.dot(pick, beams_ref[...], preferred_element_type=F32).astype(BF16)
    point = lax.broadcasted_iota(jnp.int32, (centres, live), 0) - start_ref[...]
    image = jnp.zeros((centres, DEPTH), F32)
    steps = [(ref, column) for ref, width in zip(held, widths) for column in range(width)]
    for step, (operator_ref, column) in enumerate(steps):
        if step == widths[0] + widths[1]:
            for copy in arriving:
                copy.wait()
        columns = slice(column * DEPTH, (column + 1) * DEPTH)
        footprint = jnp.dot(chosen, operator_ref[:, columns], preferred_element_type=F32)
        high, low = split_bf16(footprint)
        hit = (point == step).astype(F32).astype(BF16)
        image = image + jnp.dot(
            jnp.concatenate([hit, hit], axis=1),
            jnp.concatenate([high, low], axis=0),
            preferred_element_type=F32,
        )
    image = (image * scale).astype(BF16)
    tile = out_ref.shape[2]
    for owner in range(out_ref.shape[0]):
        for copy in range(copies):
            out_ref[owner, copy] = image[owner * tile : (owner + 1) * tile]


VMEM = pl.BlockSpec(memory_space=pltpu.VMEM)
SMEM = pl.BlockSpec(memory_space=pltpu.SMEM)
HBM = pl.BlockSpec(memory_space=pltpu.HBM)


def limit(mebibytes):
    return pltpu.CompilerParams(vmem_limit_bytes=mebibytes * 1024 * 1024)


def cost(flops, moved):
    return pl.CostEstimate(flops=flops, bytes_accessed=moved, transcendentals=0)


def in_hbm(array):
    return pltpu.with_memory_space_constraint(jnp.asarray(array), pltpu.HBM)


def shift(cells, axis, step):
    count = lax.axis_size(axis)
    return lax.ppermute(cells, axis, [(i, i + step) for i in range(count) if 0 <= i + step < count])


def beams_split_time(own, centre_offset, live_here):
    high = lax.Precision.HIGHEST
    sub_index = lax.axis_index("sub")
    samples = own.shape[1]
    freq_block = samples // 2
    sample_index = sub_index * samples + jnp.arange(samples, dtype=jnp.int32)[:, None]
    column = jnp.arange(NT, dtype=jnp.int32)[None, :]
    within = column % (2 * freq_block)
    frequency = column // (2 * freq_block) * freq_block + within % freq_block
    angle = 2.0 * math.pi / NT * (sample_index * frequency % NT).astype(F32)
    table = jnp.where(within // freq_block == 1, -jnp.sin(angle), jnp.cos(angle)) / math.sqrt(NT)
    partial_value = jnp.dot(own.astype(F32), table, precision=high)
    spectrum = lax.psum_scatter(partial_value, "sub", scatter_dimension=1, tiled=True)
    above = shift(spectrum[spectrum.shape[0] - HALF :], "mid", 1)
    below = shift(spectrum[:HALF], "mid", -1)
    padded = jnp.concatenate([above, spectrum, below], axis=0)
    windows = padded[centre_offset[:, None] + jnp.arange(2 * HALF + 1, dtype=jnp.int32)[None, :]]
    real, imag = windows[:, :, :freq_block], windows[:, :, freq_block:]
    offsets = np.arange(-HALF, HALF + 1)
    taper = jnp.asarray(offset_taper(offsets).astype(np.float32))[None, :, None]
    slopes = (0.25 * (np.arange(P_SIZE) - 0.5 * (P_SIZE - 1))).astype(np.float32)
    own_freq = (sub_index * freq_block + jnp.arange(freq_block, dtype=jnp.int32)).astype(F32)
    scale = (2.0 * math.pi / NT * slopes[:, None, None] * offsets[None, :, None]).astype(np.float32)
    theta = scale * own_freq[None, None, :]
    cosine, sine = taper * jnp.cos(theta), taper * jnp.sin(theta)
    add = functools.partial(jnp.einsum, "pxf,bxf->pbf", precision=high)
    beams = jnp.concatenate([add(cosine, real) + add(sine, imag), add(cosine, imag) - add(sine, real)], axis=2)
    alive = jnp.arange(CB_DEV, dtype=jnp.int32) < live_here
    return jnp.where(alive[None, :, None], beams, 0.0).astype(BF16)


def shards(traces, centre_offset, foot_start, beam_count, operator):
    mid_count = lax.axis_size("mid")
    off_count = lax.axis_size("off")
    sub_count = lax.axis_size("sub")
    mid_index = lax.axis_index("mid")
    samples = traces.shape[2]
    own = traces[0]
    counts = beam_count.astype(jnp.int32)
    tiles = jnp.arange(mid_count, dtype=jnp.int32)
    rows = mid_count * CB_DEV
    live_total = rows // 2
    steps = operator.shape[1] // DEPTH
    early_width, middle_width = (steps * share // 8 * DEPTH for share in SHARES)
    if sub_count == 1:
        odd_tile = mid_index % 2 == 1
        head, tail = own[:HALF], own[own.shape[0] - HALF :]
        ends = [(0, 0), (mid_count - 1, mid_count - 1)]
        inner_pairs = [(i, i - 1 if i % 2 == 0 else i + 1) for i in range(1, mid_count - 1)]
        within = lax.ppermute(jnp.where(odd_tile, head, tail), "mid", [(i, i ^ 1) for i in range(mid_count)])
        across = lax.ppermute(jnp.where(odd_tile, tail, head), "mid", ends + inner_pairs)
        tables = quarter_table() + slant_tables()
        parts = samples // LANES
        inner = own.shape[0] * parts
        edge = 2 * HALF * parts
        spec, high, low, cosine, sine, early, place, live_starts, count_held, centre_held = pl.pallas_call(
            first_stage,
            out_shape=[pltpu.VMEM((inner, LANES), F32)]
            + [pltpu.VMEM(t.shape, t.dtype) for t in tables]
            + [pltpu.VMEM((samples, early_width), BF16)]
            + [pltpu.VMEM((1, n), jnp.int32) for n in (rows, live_total)]
            + [pltpu.SMEM(t.shape, jnp.int32) for t in (counts, centre_offset)],
            in_specs=[HBM] * 9,
            out_specs=[VMEM] * 8 + [SMEM] * 2,
            scratch_shapes=[
                pltpu.VMEM(own.shape, BF16),
                pltpu.VMEM((P_SIZE, rows), jnp.int32),
                pltpu.SemaphoreType.DMA((8 + PIECES,)),
            ],
            compiler_params=limit(16),
            cost_estimate=cost(4 * 10**9, 10**7),
            name="first",
        )(*(in_hbm(t) for t in (own,) + tables[:2] + (counts, foot_start.T, centre_offset) + tables[2:] + (operator,)))
        beams, middle = pl.pallas_call(
            functools.partial(beams_stage, first_column=early_width),
            out_shape=[pltpu.VMEM((mid_count, CB_DEV, samples), BF16), pltpu.VMEM((samples, middle_width), BF16)],
            in_specs=[SMEM, SMEM, HBM] + [VMEM] * 7,
            out_specs=[VMEM] * 2,
            scratch_shapes=[
                pltpu.VMEM((edge, LANES), F32),
                pltpu.VMEM((edge + inner, LANES), F32),
                pltpu.VMEM((P_SIZE, CB_DEV * parts, LANES), F32),
                pltpu.SemaphoreType.DMA((PIECES,)),
            ],
            compiler_params=limit(16),
            cost_estimate=cost(4 * 10**9, 4 * 10**6),
            name="beams",
        )(centre_held, count_held, in_hbm(operator), spec, within, across, high, low, cosine, sine)
    else:
        live_here = jnp.sum(jnp.where(tiles == mid_index, counts, 0))
        order = np.array(travel_order(mid_count))
        beams = beams_split_time(own, centre_offset, live_here)[order // (mid_count // P_SIZE)]
        early, middle = operator[:, :early_width], operator[:, early_width : early_width + middle_width]
        first_column = mid_index * operator.shape[1]
        before = jnp.sum(jnp.where(tiles[None, :] < tiles[:, None], counts[None, :], 0), axis=1)
        slot = jnp.arange(CB_DEV, dtype=jnp.int32)
        place = jnp.where(slot[None, :] < counts[:, None], before[:, None] + slot[None, :], -1).reshape(1, rows)
        starts = lax.dynamic_index_in_dim(foot_start, first_column // (FL * DEPTH), 1, keepdims=False)
        position = jnp.arange(live_total, dtype=jnp.int32)
        here = place.reshape(rows, 1) == position[None, :]
        live_starts = jnp.sum(jnp.where(here, starts[:, None], 0), axis=0)
        live_starts = (live_starts + first_column % (FL * DEPTH) // DEPTH).reshape(1, live_total)
        place = place.reshape(mid_count, CB_DEV)[order].reshape(1, rows)
    received = lax.all_to_all(
        beams.reshape(rows, samples),
        "mid",
        split_axis=0,
        concat_axis=0,
        tiled=True,
        axis_index_groups=[travel_order(mid_count)],
    )
    partial_image = pl.pallas_call(
        functools.partial(image_stage, scale=1.0 / math.sqrt(FL * P_SIZE), copies=off_count),
        out_shape=jax.ShapeDtypeStruct((mid_count, off_count, CB_DEV, DEPTH), BF16),
        in_specs=[VMEM] * 5 + [HBM],
        out_specs=VMEM,
        scratch_shapes=[
            pltpu.VMEM((samples, operator.shape[1] - early_width - middle_width), BF16),
            pltpu.SemaphoreType.DMA((PIECES,)),
        ],
        compiler_params=limit(24),
        cost_estimate=cost(2 * 10**9, 10**7),
        name="image",
    )(place, live_starts, received, early, middle, in_hbm(operator))
    parts = lax.all_to_all(
        partial_image.reshape(mid_count * off_count * CB_DEV, DEPTH),
        ("mid", "off"),
        split_axis=0,
        concat_axis=0,
        tiled=True,
    )
    image = jnp.sum(parts.reshape(mid_count * off_count, CB_DEV, DEPTH).astype(F32), axis=0)
    if sub_count > 1:
        image = lax.psum(image, "sub")
    return image


def solution(mesh):
    return jax.shard_map(
        shards,
        mesh=mesh,
        in_specs=(
            P("off", ("grp", "mid"), "sub"),
            P(("grp", "mid")),
            P("grp", None),
            P("grp"),
            P("sub", "mid"),
        ),
        out_specs=P(("grp", "mid"), None),
        check_vma=False,
    )
```
